16 devices in a mesh: dp: 2 (over y, z), ctx: 8 (over x, core).
Axes of the slice: x: 4, y: 2, z: 1, core: 2. Of those that a mesh axis runs over, the one named last changes fastest.
The devices are a block of a 4x4x8 slice.
Arguments:
- hidden: bfloat16 [512, 2048], P(('dp', 'ctx')), parts along dimension 0
- w_q: bfloat16 [2048, 3072], replicated
- w_uk: bfloat16 [16, 128, 512], replicated
- w_uv: bfloat16 [16, 512, 128], replicated
- w_o: bfloat16 [2048, 2048], replicated
- kv_prefix: bfloat16 [32768, 576], P(('dp', 'ctx')), parts along dimension 0
- kv_suffix: bfloat16 [512, 2048, 576], P(('dp', 'ctx')), parts along dimension 0
- seq_lens: int32 [512], P(('dp', 'ctx')), parts along dimension 0
Outputs:
- output: bfloat16 [512, 2048], P(('dp', 'ctx')), parts along dimension 0
There are 2 independent parts. The reference program is written for one: setup_inputs(seed, part) draws one part's arguments, and reference() takes and returns one part's arrays. A program takes and returns all parts, laid end to end along the dimension named above; an argument that names none is the same for every part.
All inputs are finite; a program needn't handle non-finite values.
Results may differ from the reference program's by a relative error of at most 0.00657954.
Values are sent between devices in bfloat16 or wider.
A program may use at most 768 MiB of HBM per device.

```python
import math
import jax
import jax.numpy as jnp
from jax import lax

MODEL_DIM = 2048
HEADS = 16
NOPE_DIM = 128
ROPE_DIM = 64
VALUE_DIM = 128
LATENT_DIM = 512
GROUP_SIZE = 8
SEQUENCES = 256
PREFIX_LEN = 16384
SUFFIX_LEN = 2048
ROPE_BASE = 10000

KV_WIDTH = LATENT_DIM + ROPE_DIM
QK_WIDTH = NOPE_DIM + ROPE_DIM
SCORE_SCALE = QK_WIDTH ** -0.5
BLOCK_LEN = PREFIX_LEN // GROUP_SIZE
PREFIX_AMP = 1.5
SUFFIX_AMP = PREFIX_AMP * math.sqrt(1.0 + 2.0 * math.log(max(2.0 * PREFIX_LEN / SUFFIX_LEN, 1.0)) * QK_WIDTH / (PREFIX_AMP ** 2 * LATENT_DIM))


def draw_lengths(key):
    raw_lens = jax.random.randint(key, (SEQUENCES,), 0, SUFFIX_LEN, jnp.int32)
    seq_index = jnp.arange(SEQUENCES)
    return jnp.where(seq_index == 0, SUFFIX_LEN - 1, jnp.where(seq_index == 1, 0, raw_lens)).astype(jnp.int32)


def latent_cache(noise, means):
    rope_pad = jnp.zeros(means.shape[:-1] + (ROPE_DIM,), jnp.float32)
    return noise + jnp.concatenate([means, rope_pad], axis=-1)


def setup_inputs(seed: int = 0, part: int = 0) -> dict:
    shared_keys = jax.random.split(jax.random.key(seed + 1), 4)
    own_keys = jax.random.split(jax.random.fold_in(jax.random.key(seed), part), 6)
    hidden = jax.random.normal(own_keys[0], (SEQUENCES, MODEL_DIM), jnp.float32)
    w_q = jax.random.normal(shared_keys[0], (MODEL_DIM, HEADS * QK_WIDTH), jnp.float32) * MODEL_DIM ** -0.5
    w_uk = jax.random.normal(shared_keys[1], (HEADS, NOPE_DIM, LATENT_DIM), jnp.float32) * NOPE_DIM ** -0.5
    w_uv = jax.random.normal(shared_keys[2], (HEADS, LATENT_DIM, VALUE_DIM), jnp.float32) * LATENT_DIM ** -0.5
    w_o = jax.random.normal(shared_keys[3], (HEADS * VALUE_DIM, MODEL_DIM), jnp.float32) * (HEADS * VALUE_DIM) ** -0.5
    pre_noise = jax.random.normal(own_keys[1], (GROUP_SIZE, BLOCK_LEN, KV_WIDTH), jnp.float32)
    pre_means = jax.random.normal(own_keys[2], (GROUP_SIZE, 1, LATENT_DIM), jnp.float32) * PREFIX_AMP
    kv_prefix = latent_cache(pre_noise, pre_means).reshape(PREFIX_LEN, KV_WIDTH)
    suf_noise = jax.random.normal(own_keys[3], (SEQUENCES, SUFFIX_LEN, KV_WIDTH), jnp.float32)
    suf_means = jax.random.normal(own_keys[4], (SEQUENCES, 1, LATENT_DIM), jnp.float32) * SUFFIX_AMP
    kv_suffix = latent_cache(suf_noise, suf_means)
    seq_lens = draw_lengths(own_keys[5])
    return {'hidden': hidden.astype(jnp.bfloat16), 'w_q': w_q.astype(jnp.bfloat16), 'w_uk': w_uk.astype(jnp.bfloat16), 'w_uv': w_uv.astype(jnp.bfloat16), 'w_o': w_o.astype(jnp.bfloat16), 'kv_prefix': kv_prefix.astype(jnp.bfloat16), 'kv_suffix': kv_suffix.astype(jnp.bfloat16), 'seq_lens': seq_lens}


def rope_rotate(rot_in, positions):
    half_dim = ROPE_DIM // 2
    inv_freq = jnp.exp(jnp.arange(half_dim, dtype=jnp.float32) * (-math.log(ROPE_BASE) / half_dim))
    angle = positions.astype(jnp.float32)[:, None, None] * inv_freq
    cos_part = jnp.cos(angle)
    sin_part = jnp.sin(angle)
    rot_wide = rot_in.astype(jnp.float32)
    first_half = rot_wide[..., :half_dim]
    second_half = rot_wide[..., half_dim:]
    return jnp.concatenate([first_half * cos_part - second_half * sin_part, second_half * cos_part + first_half * sin_part], axis=-1)


def reference(hidden, w_q, w_uk, w_uv, w_o, kv_prefix, kv_suffix, seq_lens):
    q_all = jnp.dot(hidden, w_q, preferred_element_type=jnp.float32).astype(jnp.bfloat16).reshape(SEQUENCES, HEADS, QK_WIDTH)
    q_lat = jnp.einsum('bhn,hnc->bhc', q_all[..., :NOPE_DIM].astype(jnp.float32), w_uk.astype(jnp.float32)).astype(jnp.bfloat16)
    q_rot = rope_rotate(q_all[..., NOPE_DIM:], PREFIX_LEN + seq_lens).astype(jnp.bfloat16)
    query = jnp.concatenate([q_lat, q_rot], axis=-1)
    pre_keys = kv_prefix.astype(jnp.float32)
    pre_vals = pre_keys[:, :LATENT_DIM]
    slots = jnp.arange(SUFFIX_LEN)

    def one_sequence(item):
        q_row, suf_row, length = item
        q_row = q_row.astype(jnp.float32)
        suf_keys = suf_row.astype(jnp.float32)
        s_pre = jnp.einsum('hw,pw->hp', q_row, pre_keys) * SCORE_SCALE
        s_suf = jnp.einsum('hw,sw->hs', q_row, suf_keys) * SCORE_SCALE
        s_suf = jnp.where((slots <= length)[None, :], s_suf, -jnp.inf)
        probs = jax.nn.softmax(jnp.concatenate([s_pre, s_suf], axis=-1), axis=-1)
        return jnp.dot(probs[:, :PREFIX_LEN], pre_vals) + jnp.dot(probs[:, PREFIX_LEN:], suf_keys[:, :LATENT_DIM])

    o_lat = lax.map(one_sequence, (query, kv_suffix, seq_lens)).astype(jnp.bfloat16)
    o_val = jnp.einsum('bhc,hcv->bhv', o_lat.astype(jnp.float32), w_uv.astype(jnp.float32)).astype(jnp.bfloat16)
    out = hidden.astype(jnp.float32) + jnp.dot(o_val.reshape(SEQUENCES, HEADS * VALUE_DIM), w_o, preferred_element_type=jnp.float32)
    return out.astype(jnp.bfloat16)
```

```python
import functools
import math
import jax
import jax.numpy as jnp
from jax import lax
from jax.experimental import pallas as pl
from jax.experimental.pallas import tpu as pltpu
from jax.sharding import PartitionSpec as P

ROPE_BASE = 10000
LOG2E = math.log2(math.e)
CORES = 2
F32 = jnp.float32
BF16 = jnp.bfloat16
ANY = pl.BlockSpec(memory_space=pl.ANY)
VMEM = pl.BlockSpec(memory_space=pltpu.VMEM)
SMEM = pl.BlockSpec(memory_space=pltpu.SMEM)
NT = (((1,), (1,)), ((), ()))


def rope_table(positions, half_dim):
    inv_freq = jnp.exp(jnp.arange(half_dim, dtype=F32) * (-math.log(ROPE_BASE) / half_dim))
    angle = positions.astype(F32)[:, None] * inv_freq
    cos_part = jnp.cos(angle)
    sin_part = jnp.sin(angle)
    return jnp.concatenate([cos_part, cos_part, sin_part, sin_part], axis=-1)


def query_kernel(chips, hid_ref, cs_ref, wq_hbm, wuk_hbm, kv_hbm, q_ref, kvo_hbm,
                 hid_all, cs_all, wq_buf, wuk_buf, wq_sem, wuk_sem, send_sem, recv_sem, cs_send, cs_recv, kv_send, kv_recv):
    me = lax.axis_index('ctx')
    group = chips * CORES
    chip, core = me // CORES, me % CORES
    steps = wq_buf.shape[0]
    wide = wq_buf.shape[2]
    rows = hid_ref.shape[0]
    nope, lat = wuk_buf.shape[1], wuk_buf.shape[2]
    rope = q_ref.shape[2] - lat
    head_w = nope + rope
    per = wide // head_w
    for i in range(steps):
        pltpu.make_async_copy(wq_hbm.at[:, pl.ds(i * wide, wide)], wq_buf.at[i], wq_sem.at[i]).start()
    uk_copy = pltpu.make_async_copy(wuk_hbm, wuk_buf, wuk_sem)
    uk_copy.start()
    partner = chip * CORES + (1 - core)
    peers = [((chip + chips - r) % chips) * CORES + core for r in range(1, chips)]
    barrier = pltpu.get_barrier_semaphore()
    for dev in [partner] + peers:
        pl.semaphore_signal(barrier, inc=1, device_id={'ctx': dev}, device_id_type=pl.DeviceIdType.MESH)
    pl.semaphore_wait(barrier, chips)
    copies = []
    for r in range(1, chips):
        dst = {'ctx': peers[r - 1]}
        copies.append(pltpu.make_async_remote_copy(hid_ref, hid_all.at[r], send_sem.at[r], recv_sem.at[r], device_id=dst, device_id_type=pl.DeviceIdType.MESH))
        copies.append(pltpu.make_async_remote_copy(cs_ref, cs_all.at[r], cs_send.at[r], cs_recv.at[r], device_id=dst, device_id_type=pl.DeviceIdType.MESH))
    for c in copies:
        c.start()
    kv_copy = pltpu.make_async_remote_copy(kv_hbm, kvo_hbm, kv_send, kv_recv, device_id={'ctx': partner}, device_id_type=pl.DeviceIdType.MESH)
    kv_copy.start()
    hid_all[0] = hid_ref[...]
    cs_all[0] = cs_ref[...]
    for c in copies:
        c.wait()
    uk_copy.wait()
    x = hid_all[...].reshape(chips * rows, hid_ref.shape[1])
    cs = cs_all[...].reshape(chips * rows, 2 * rope)
    cos, sin = cs[:, :rope], cs[:, rope:]
    for i in range(steps):
        pltpu.make_async_copy(wq_hbm.at[:, pl.ds(i * wide, wide)], wq_buf.at[i], wq_sem.at[i]).wait()
        qa = jnp.dot(x, wq_buf[i], preferred_element_type=F32).astype(BF16)
        for k in range(per):
            h = i * per + k
            q_lat = jnp.dot(qa[:, k * head_w:k * head_w + nope], wuk_buf[h], preferred_element_type=F32)
            q_ref[h, :, 0:lat] = q_lat.astype(BF16)
            pe = qa[:, k * head_w + nope:(k + 1) * head_w].astype(F32)
            turned = jnp.concatenate([-pe[:, rope // 2:], pe[:, :rope // 2]], axis=1)
            q_ref[h, :, lat:lat + rope] = (pe * cos + turned * sin).astype(BF16)
    kv_copy.wait()


def gather_queries(hidden, cs, w_q, w_uk, kv_prefix, chips):
    rows, depth = hidden.shape
    heads, nope, lat = w_uk.shape
    head_w = w_q.shape[1] // heads
    rope = head_w - nope
    steps = 4
    wide = w_q.shape[1] // steps
    return pl.pallas_call(
        functools.partial(query_kernel, chips),
        out_shape=[jax.ShapeDtypeStruct((heads, chips * rows, lat + rope), BF16), jax.ShapeDtypeStruct(kv_prefix.shape, BF16)],
        in_specs=[VMEM, VMEM, ANY, ANY, ANY],
        out_specs=[VMEM, ANY],
        scratch_shapes=[
            pltpu.VMEM((chips, rows, depth), BF16), pltpu.VMEM((chips, rows, 2 * rope), F32),
            pltpu.VMEM((steps, depth, wide), BF16), pltpu.VMEM(w_uk.shape, BF16),
            pltpu.SemaphoreType.DMA((steps,)), pltpu.SemaphoreType.DMA,
            pltpu.SemaphoreType.DMA((chips,)), pltpu.SemaphoreType.DMA((chips,)),
            pltpu.SemaphoreType.DMA((chips,)), pltpu.SemaphoreType.DMA((chips,)),
            pltpu.SemaphoreType.DMA, pltpu.SemaphoreType.DMA],
        compiler_params=pltpu.CompilerParams(collective_id=0, has_side_effects=True, vmem_limit_bytes=48 * 2**20),
        name='gather_queries',
    )(hidden, cs, w_q, w_uk, kv_prefix)


def prefix_kernel(scale2, lat, sub, q_ref, ka_ref, kb_ref, oa_ref, ob_ref, acc_ref, m_ref, l_ref):
    step = pl.program_id(0)
    rows = q_ref.shape[0]

    @pl.when(step == 0)
    def _():
        m_ref[...] = jnp.full_like(m_ref, -jnp.inf)
        l_ref[...] = jnp.zeros_like(l_ref)
        acc_ref[...] = jnp.zeros_like(acc_ref)

    parts = [(ref, i) for i in range(ka_ref.shape[1] // sub) for ref in (ka_ref, kb_ref)]

    def scores(ref, i):
        return jnp.dot(q_ref[...], ref[:, i * sub:(i + 1) * sub], preferred_element_type=F32)

    s_now = scores(*parts[0])
    for n, (ref, i) in enumerate(parts):
        s_next = scores(*parts[n + 1]) if n + 1 < len(parts) else None
        s2 = s_now * scale2
        m_old = m_ref[...]
        m_new = jnp.maximum(m_old, jnp.max(s2, axis=1, keepdims=True))
        alpha = jnp.exp2(m_old - m_new)
        p = jnp.exp2(s2 - m_new[:, :1])
        part_l = p[:, 0:128]
        for k in range(1, sub // 128):
            part_l = part_l + p[:, k * 128:(k + 1) * 128]
        l_ref[...] = l_ref[...] * alpha + part_l
        m_ref[...] = m_new
        pv = lax.dot_general(p.astype(BF16), ref[0:lat, i * sub:(i + 1) * sub], NT, preferred_element_type=F32)
        acc_ref[...] = acc_ref[...] * alpha[:, :1] + pv
        s_now = s_next

    @pl.when(step == pl.num_programs(0) - 1)
    def _():
        half = rows // 2
        m_t = m_ref[...].T[0:8]
        l_sum = jnp.sum(l_ref[...], axis=1, keepdims=True)
        l_t = jnp.broadcast_to(l_sum, (rows, 128)).T[0:8]
        for k, ref in enumerate((oa_ref, ob_ref)):
            ref[0:half, :] = acc_ref[k * half:(k + 1) * half, :]
            ref[half:half + 8, 0:half] = m_t[:, k * half:(k + 1) * half]
            ref[half:half + 8, half:2 * half] = l_t[:, k * half:(k + 1) * half]


def prefix_part(q_rows, kv_a, kv_b, scale2, lat, name):
    rows, width = q_rows.shape
    half = rows // 2
    block, sub = 512, 512
    grid = kv_a.shape[1] // block
    kv_spec = pl.BlockSpec((width, block), lambda j: (0, j))
    out = jax.ShapeDtypeStruct((half + 8, lat), F32)
    keys = 2 * kv_a.shape[1]
    return pl.pallas_call(
        functools.partial(prefix_kernel, scale2, lat, sub),
        out_shape=[out, out],
        grid=(grid,),
        in_specs=[pl.BlockSpec((rows, width), lambda j: (0, 0)), kv_spec, kv_spec],
        out_specs=[pl.BlockSpec((half + 8, lat), lambda j: (0, 0))] * 2,
        scratch_shapes=[pltpu.VMEM((rows, lat), F32), pltpu.VMEM((rows, 128), F32), pltpu.VMEM((rows, 128), F32)],
        compiler_params=pltpu.CompilerParams(dimension_semantics=('arbitrary',), vmem_limit_bytes=40 * 2**20),
        cost_estimate=pl.CostEstimate(flops=2 * rows * keys * (768 + lat), bytes_accessed=keys * width * 2, transcendentals=rows * keys),
        name=name,
    )(q_rows, kv_a, kv_b)


def suffix_kernel(scale2, lat, lens_ref, q_ref, kv_hbm, o_ref, m_out, l_out, bufs, sems):
    seqs, heads = q_ref.shape[0], q_ref.shape[1]
    depth, size = bufs.shape[0], bufs.shape[2]

    def count(b, total):
        return total + lens_ref[b] // size + 1

    total = lax.fori_loop(0, seqs, count, 0)

    def advance(b, j):
        last = j >= lens_ref[jnp.minimum(b, seqs - 1)] // size
        return jnp.where(last, b + 1, b), jnp.where(last, 0, j + 1)

    def copy(b, j, slot):
        return pltpu.make_async_copy(kv_hbm.at[b, :, pl.ds(pl.multiple_of(j * size, size), size)], bufs.at[slot], sems.at[slot])

    def scores(b, slot):
        return jnp.dot(q_ref[jnp.minimum(b, seqs - 1)], bufs[slot], preferred_element_type=F32)

    b, j = 0, 0
    for n in range(depth - 1):
        copy(b, j, n).start()
        b, j = advance(jnp.int32(b), jnp.int32(j))
    dma = (b, j)
    zero = jnp.int32(0)
    copy(0, 0, 0).wait()
    s0 = scores(zero, 0)
    nxt = advance(zero, zero)
    pos = lax.broadcasted_iota(jnp.int32, (heads, size), 1)

    def body(t, carry):
        bc, jc, bn, jn, bd, jd, s_now, m, l, acc = carry

        @pl.when(t + depth - 1 < total)
        def _():
            copy(bd, jd, (t + depth - 1) % depth).start()

        @pl.when(t + 1 < total)
        def _():
            copy(bn, jn, (t + 1) % depth).wait()

        s_next = scores(bn, (t + 1) % depth)
        s2 = jnp.where(pos <= lens_ref[bc] - jc * size, s_now * scale2, -jnp.inf)
        m_old = jnp.where(jc == 0, -jnp.inf, m)
        m_new = jnp.maximum(m_old, jnp.max(s2, axis=1, keepdims=True))
        alpha = jnp.exp2(m_old - m_new)
        p = jnp.exp2(s2 - m_new[:, :1])
        l_new = l * alpha + jnp.sum(p, axis=1, keepdims=True)
        pv = lax.dot_general(p.astype(BF16), bufs[t % depth, 0:lat, :], NT, preferred_element_type=F32)
        acc_new = acc * alpha[:, :1] + pv
        o_ref[bc] = acc_new
        m_out[bc] = m_new
        l_out[bc] = l_new
        bd2, jd2 = advance(bd, jd)
        bn2, jn2 = advance(bn, jn)
        return bn, jn, bn2, jn2, bd2, jd2, s_next, m_new, l_new, acc_new

    stat = jnp.zeros((heads, 128), F32)
    lax.fori_loop(0, total, body, (zero, zero, nxt[0], nxt[1], dma[0], dma[1], s0, stat, stat, jnp.zeros((heads, lat), F32)))


def suffix_part(query, kv_suffix, seq_lens, scale2, lat):
    seqs, heads, width = query.shape
    size, depth = 512, 4
    slots = kv_suffix.shape[2]
    return pl.pallas_call(
        functools.partial(suffix_kernel, scale2, lat),
        out_shape=[jax.ShapeDtypeStruct((seqs, heads, lat), F32), jax.ShapeDtypeStruct((seqs, heads, 128), F32), jax.ShapeDtypeStruct((seqs, heads, 128), F32)],
        in_specs=[SMEM, VMEM, ANY],
        out_specs=[VMEM, VMEM, VMEM],
        scratch_shapes=[pltpu.VMEM((depth, width, size), BF16), pltpu.SemaphoreType.DMA((depth,))],
        compiler_params=pltpu.CompilerParams(vmem_limit_bytes=40 * 2**20),
        cost_estimate=pl.CostEstimate(flops=2 * seqs * slots * 256 * 768, bytes_accessed=seqs * slots * width * 2, transcendentals=seqs * slots * heads),
        name='suffix',
    )(seq_lens, query, kv_suffix)


def read_part(ref):
    half = ref.shape[0] - 8
    stats = ref[half:half + 8, :]
    return ref[0:half, :], stats[:, 0:half].T[:, 0:1], stats[:, half:2 * half].T[:, 0:1]


def merge(parts):
    m_all = functools.reduce(jnp.maximum, [m for _, m, _ in parts])
    weights = [jnp.exp2(m - m_all) for _, m, _ in parts]
    o_all = functools.reduce(jnp.add, [o * w for (o, _, _), w in zip(parts, weights)])
    l_all = functools.reduce(jnp.add, [l * w for (_, _, l), w in zip(parts, weights)])
    return o_all, m_all, l_all


def merge_kernel(x_ref, y_ref, o_ref):
    half = x_ref.shape[0] - 8
    o_all, m_all, l_all = merge([read_part(x_ref), read_part(y_ref)])
    o_ref[0:half, :] = o_all
    o_ref[half:half + 8, 0:half] = jnp.broadcast_to(m_all, (half, 128)).T[0:8]
    o_ref[half:half + 8, half:2 * half] = jnp.broadcast_to(l_all, (half, 128)).T[0:8]


def merge_parts(x, y, name):
    return pl.pallas_call(
        merge_kernel,
        out_shape=jax.ShapeDtypeStruct(x.shape, F32),
        in_specs=[VMEM, VMEM],
        out_specs=VMEM,
        compiler_params=pltpu.CompilerParams(vmem_limit_bytes=8 * 2**20),
        cost_estimate=pl.CostEstimate(flops=4 * x.size, bytes_accessed=12 * x.size, transcendentals=0),
        name=name,
    )(x, y)


def output_kernel(hid_ref, os_ref, ms_ref, ls_ref, *refs):
    parts, (uv_ref, wo_ref, out_ref, o_buf, v_buf) = refs[:6], refs[6:]
    rows, heads = hid_ref.shape[0], uv_ref.shape[0]
    half = parts[0].shape[0] - 8
    for k in range(2):
        cut = slice(k * half, (k + 1) * half)
        pieces = [(os_ref[cut, :], ms_ref[cut, 0:1], ls_ref[cut, 0:1])] + [read_part(ref) for ref in parts[3 * k:3 * k + 3]]
        o_all, _, l_all = merge(pieces)
        o_all = o_all / l_all
        for n in range(o_buf.shape[0]):
            o_buf[n, cut, :] = o_all[:, n * 128:(n + 1) * 128]
    width = uv_ref.shape[2]
    for h in range(heads):
        o_h = jnp.concatenate([o_buf[n, pl.ds(h, rows, stride=heads), :] for n in range(o_buf.shape[0])], axis=1).astype(BF16)
        v_buf[:, h * width:(h + 1) * width] = jnp.dot(o_h, uv_ref[h], preferred_element_type=F32).astype(BF16)
    proj = jnp.dot(v_buf[...], wo_ref[...], preferred_element_type=F32)
    out_ref[...] = (hid_ref[...].astype(F32) + proj).astype(BF16)


def output_part(hidden, o_s, m_s, l_s, parts, w_uv, w_o):
    rows = hidden.shape[0]
    heads, lat, val = w_uv.shape
    return pl.pallas_call(
        output_kernel,
        out_shape=jax.ShapeDtypeStruct(hidden.shape, BF16),
        in_specs=[VMEM] * 12,
        out_specs=VMEM,
        scratch_shapes=[pltpu.VMEM((lat // 128, rows * heads, 128), F32), pltpu.VMEM((rows, heads * val), BF16)],
        compiler_params=pltpu.CompilerParams(vmem_limit_bytes=24 * 2**20),
        cost_estimate=pl.CostEstimate(flops=2 * rows * heads * val * (lat + hidden.shape[1]), bytes_accessed=2 * (w_uv.size + w_o.size), transcendentals=0),
        name='output',
    )(hidden, o_s, m_s, l_s, *parts, w_uv, w_o)


def solution(mesh):
    group = mesh.shape['ctx']
    chips = group // CORES
    rows_spec = P(('dp', 'ctx'), None)
    whole_spec = P()

    def local_step(hidden, w_q, w_uk, w_uv, w_o, kv_prefix, kv_suffix, seq_lens):
        rows = hidden.shape[0]
        heads, nope, lat = w_uk.shape
        head_w = w_q.shape[1] // heads
        rope = head_w - nope
        prefix_len = kv_prefix.shape[0] * group
        scale2 = head_w ** -0.5 * LOG2E
        kv_prefix = kv_prefix.T
        kv_suffix = kv_suffix.transpose(0, 2, 1)
        cs = rope_table(prefix_len + seq_lens, rope // 2)
        q_all, kv_other = gather_queries(hidden, cs, w_q, w_uk, kv_prefix, chips)
        q_all = q_all.reshape(heads, chips, rows, -1).transpose(1, 2, 0, 3)

        def send(value, hop):
            return lax.ppermute(value, 'ctx', [(j, (j + hop * CORES) % group) for j in range(group)])

        def part(query, name):
            return prefix_part(query.reshape(rows * heads, -1), kv_prefix, kv_other, scale2, lat, name)

        def after(value, *earlier):
            return lax.optimization_barrier((value,) + earlier)[0]

        far_a, far_b = part(q_all[2], 'prefix_far')
        got_a = send(far_a, 1)
        got_b = send(far_b, -1)
        up_a, up_b = part(after(q_all[1], far_a, far_b), 'prefix_up')
        in_up_b = send(up_b, 1)
        down_a, down_b = part(after(q_all[3], up_a, up_b), 'prefix_down')
        in_down_a = send(down_a, -1)
        up_m = merge_parts(up_a, got_a, 'merge_up')
        in_up_a = send(up_m, 1)
        down_m = merge_parts(after(down_b, up_m), got_b, 'merge_down')
        in_down_b = send(down_m, -1)
        own_a, own_b = part(after(q_all[0], down_m), 'prefix_own')
        o_s, m_s, l_s = suffix_part(after(q_all[0], own_a, own_b), kv_suffix, seq_lens, scale2, lat)
        flat = rows * heads
        o_s, m_s, l_s = o_s.reshape(flat, lat), m_s.reshape(flat, 128), l_s.reshape(flat, 128)
        parts = (own_a, in_up_a, in_down_a, own_b, in_up_b, in_down_b)
        return output_part(hidden, o_s, m_s, l_s, parts, w_uv, w_o)

    return jax.shard_map(local_step, mesh=mesh, in_specs=(rows_spec, whole_spec, whole_spec, whole_spec, whole_spec, rows_spec, P(('dp', 'ctx'), None, None), P(('dp', 'ctx'))), out_specs=rows_spec, check_vma=False)
```

```python
import functools
import math
import jax
import jax.numpy as jnp
from jax import lax
from jax.experimental import pallas as pl
from jax.experimental.pallas import tpu as pltpu
from jax.sharding import PartitionSpec as P

ROPE_BASE = 10000
LOG2E = math.log2(math.e)
CORES = 2
F32 = jnp.float32
BF16 = jnp.bfloat16
HBM = pl.BlockSpec(memory_space=pltpu.HBM)
VMEM = pl.BlockSpec(memory_space=pltpu.VMEM)
SMEM = pl.BlockSpec(memory_space=pltpu.SMEM)
NT = (((1,), (1,)), ((), ()))


def rope_table(positions, half_dim):
    inv_freq = jnp.exp(jnp.arange(half_dim, dtype=F32) * (-math.log(ROPE_BASE) / half_dim))
    angle = positions.astype(F32)[:, None] * inv_freq
    cos_part = jnp.cos(angle)
    sin_part = jnp.sin(angle)
    return jnp.concatenate([cos_part, cos_part, sin_part, sin_part], axis=-1)


def query_kernel(chips, hid_ref, cs_ref, wq_hbm, wuk_hbm, kv_hbm, q_ref, k_ref,
                 hid_all, cs_all, wq_buf, wuk_buf, wq_sem, wuk_sem, send_sem, recv_sem, cs_send, cs_recv, kv_send, kv_recv, kv_sem):
    me = lax.axis_index('ctx')
    group = chips * CORES
    chip, core = me // CORES, me % CORES
    steps = wq_buf.shape[0]
    wide = wq_buf.shape[2]
    rows = hid_ref.shape[0]
    nope, lat = wuk_buf.shape[1], wuk_buf.shape[2]
    rope = q_ref.shape[3] - lat
    head_w = nope + rope
    keys = kv_hbm.shape[1]
    per = wide // head_w
    for i in range(steps):
        pltpu.make_async_copy(wq_hbm.at[:, pl.ds(i * wide, wide)], wq_buf.at[i], wq_sem.at[i]).start()
    uk_copy = pltpu.make_async_copy(wuk_hbm, wuk_buf, wuk_sem)
    uk_copy.start()
    own_copy = pltpu.make_async_copy(kv_hbm, k_ref.at[:, pl.ds(0, keys)], kv_sem)
    own_copy.start()
    partner = chip * CORES + (1 - core)
    peers = [((chip + chips - r) % chips) * CORES + core for r in range(1, chips)]
    barrier = pltpu.get_barrier_semaphore()
    for dev in [partner] + peers:
        pl.semaphore_signal(barrier, inc=1, device_id={'ctx': dev}, device_id_type=pl.DeviceIdType.MESH)
    pl.semaphore_wait(barrier, chips)
    copies = []
    for r in range(1, chips):
        dst = {'ctx': peers[r - 1]}
        copies.append(pltpu.make_async_remote_copy(hid_ref, hid_all.at[r], send_sem.at[r], recv_sem.at[r], device_id=dst, device_id_type=pl.DeviceIdType.MESH))
        copies.append(pltpu.make_async_remote_copy(cs_ref, cs_all.at[r], cs_send.at[r], cs_recv.at[r], device_id=dst, device_id_type=pl.DeviceIdType.MESH))
    for c in copies:
        c.start()
    kv_copy = pltpu.make_async_remote_copy(kv_hbm, k_ref.at[:, pl.ds(keys, keys)], kv_send, kv_recv, device_id={'ctx': partner}, device_id_type=pl.DeviceIdType.MESH)
    kv_copy.start()
    hid_all[0] = hid_ref[...]
    cs_all[0] = cs_ref[...]
    for c in copies:
        c.wait()
    uk_copy.wait()
    x = hid_all[...].reshape(chips * rows, hid_ref.shape[1])
    cs = cs_all[...].reshape(chips * rows, 2 * rope)
    cos, sin = cs[:, :rope], cs[:, rope:]
    for i in range(steps):
        pltpu.make_async_copy(wq_hbm.at[:, pl.ds(i * wide, wide)], wq_buf.at[i], wq_sem.at[i]).wait()
        qa = jnp.dot(x, wq_buf[i], preferred_element_type=F32).astype(BF16)
        for k in range(per):
            h = i * per + k
            q_lat = jnp.dot(qa[:, k * head_w:k * head_w + nope], wuk_buf[h], preferred_element_type=F32)
            q_lat = q_lat.astype(BF16)
            pe = qa[:, k * head_w + nope:(k + 1) * head_w].astype(F32)
            turned = jnp.concatenate([-pe[:, rope // 2:], pe[:, :rope // 2]], axis=1)
            pe = (pe * cos + turned * sin).astype(BF16)
            for r in range(chips):
                q_ref[r, h, :, 0:lat] = q_lat[r * rows:(r + 1) * rows]
                q_ref[r, h, :, lat:lat + rope] = pe[r * rows:(r + 1) * rows]
    own_copy.wait()
    kv_copy.wait()


def gather_queries(hidden, cs, w_q, w_uk, kv_prefix, chips):
    rows, depth = hidden.shape
    heads, nope, lat = w_uk.shape
    head_w = w_q.shape[1] // heads
    rope = head_w - nope
    steps = 4
    wide = w_q.shape[1] // steps
    return pl.pallas_call(
        functools.partial(query_kernel, chips),
        out_shape=[jax.ShapeDtypeStruct((chips, heads, rows, lat + rope), BF16), jax.ShapeDtypeStruct((kv_prefix.shape[0], CORES * kv_prefix.shape[1]), BF16)],
        in_specs=[VMEM, VMEM, HBM, HBM, HBM],
        out_specs=[VMEM, VMEM],
        scratch_shapes=[
            pltpu.VMEM((chips, rows, depth), BF16), pltpu.VMEM((chips, rows, 2 * rope), F32),
            pltpu.VMEM((steps, depth, wide), BF16), pltpu.VMEM(w_uk.shape, BF16),
            pltpu.SemaphoreType.DMA((steps,)), pltpu.SemaphoreType.DMA,
            pltpu.SemaphoreType.DMA((chips,)), pltpu.SemaphoreType.DMA((chips,)),
            pltpu.SemaphoreType.DMA((chips,)), pltpu.SemaphoreType.DMA((chips,)),
            pltpu.SemaphoreType.DMA, pltpu.SemaphoreType.DMA, pltpu.SemaphoreType.DMA],
        compiler_params=pltpu.CompilerParams(collective_id=0, has_side_effects=True, vmem_limit_bytes=54 * 2**20),
        name='gather_queries',
    )(hidden, cs, w_q, w_uk, kv_prefix)


def prefix_kernel(scale2, lat, sub, q_ref, k_ref, *refs):
    outs, (s_ref, p_ref, acc_ref, a_ref, m_ref, l_ref) = refs[:-6], refs[-6:]
    rows = q_ref.shape[0]
    count = k_ref.shape[1] // sub
    chunk = 64
    m_ref[...] = jnp.full_like(m_ref, -jnp.inf)
    l_ref[...] = jnp.zeros_like(l_ref)
    acc_ref[...] = jnp.zeros_like(acc_ref)

    def keys(n):
        return pl.ds(pl.multiple_of(n * sub, sub), sub)

    def scores(n, slot):
        s_ref[slot] = jnp.dot(q_ref[...], k_ref[:, keys(n)], preferred_element_type=F32)

    def absorb(n, slot):
        for r in range(0, rows, chunk):
            cut = slice(r, r + chunk)
            s = s_ref[slot, cut, :]
            m_old = m_ref[cut, :]
            m_new = jnp.maximum(m_old, jnp.max(s, axis=1, keepdims=True) * scale2)
            alpha = jnp.exp2(m_old - m_new)
            l_new = l_ref[cut, :] * alpha
            for k in range(0, sub, 128):
                p = jnp.exp2(s[:, k:k + 128] * scale2 - m_new)
                l_new = l_new + p
                p_ref[slot, cut, k:k + 128] = p.astype(BF16)
            l_ref[cut, :] = l_new
            m_ref[cut, :] = m_new
            a_ref[cut, :] = alpha
        pv = lax.dot_general(p_ref[slot], k_ref[0:lat, keys(n)], NT, preferred_element_type=F32)
        for r in range(0, rows, chunk):
            cut = slice(r, r + chunk)
            alpha = a_ref[cut, :]
            for k in range(0, lat, 128):
                acc_ref[cut, k:k + 128] = acc_ref[cut, k:k + 128] * alpha + pv[cut, k:k + 128]

    scores(0, 0)

    def pair(i, carry):
        scores(2 * i + 1, 1)
        absorb(2 * i, 0)
        scores(2 * i + 2, 0)
        absorb(2 * i + 1, 1)
        return carry

    lax.fori_loop(0, count // 2 - 1, pair, 0)
    scores(count - 1, 1)
    absorb(count - 2, 0)
    absorb(count - 1, 1)
    m_t = m_ref[...].T[0:1]
    l_t = jnp.broadcast_to(jnp.sum(l_ref[...], axis=1, keepdims=True), (rows, 128)).T[0:1]
    size = rows // len(outs)
    for k, ref in enumerate(outs):
        cut = slice(k * size, (k + 1) * size)
        ref[0:size, :] = acc_ref[cut, :]
        ref[size:size + 1, 0:size] = m_t[:, cut]
        ref[size + 1:size + 2, 0:size] = l_t[:, cut]


def prefix_part(q_rows, keys, scale2, lat, pieces, name):
    rows, width = q_rows.shape
    sub = 512
    total = keys.shape[1]
    out = jax.ShapeDtypeStruct((rows // pieces + 8, lat), F32)
    return pl.pallas_call(
        functools.partial(prefix_kernel, scale2, lat, sub),
        out_shape=[out] * pieces,
        in_specs=[VMEM, VMEM],
        out_specs=[VMEM] * pieces,
        scratch_shapes=[pltpu.VMEM((2, rows, sub), F32), pltpu.VMEM((2, rows, sub), BF16), pltpu.VMEM((rows, lat), F32)] + [pltpu.VMEM((rows, 128), F32)] * 3,
        compiler_params=pltpu.CompilerParams(vmem_limit_bytes=24 * 2**20),
        cost_estimate=pl.CostEstimate(flops=2 * rows * total * (768 + lat), bytes_accessed=total * width * 2, transcendentals=rows * total),
        name=name,
    )(q_rows, keys)


def suffix_kernel(scale2, lat, heads, lens_ref, q_ref, kv_hbm, o_ref, m_out, l_out, q_buf, bufs, sems):
    seqs = q_ref.shape[0] // heads
    width = q_ref.shape[1]
    depth, size = bufs.shape[0], bufs.shape[2]
    lanes = [(k, min(k + 128, width)) for k in range(0, width, 128)]
    for n, (lo, hi) in enumerate(lanes):
        q_buf[n, :, 0:hi - lo] = q_ref[:, lo:hi].astype(F32)

    total = lax.fori_loop(0, seqs, lambda b, n: n + lens_ref[b] // size + 1, 0)

    def advance(b, j):
        last = j >= lens_ref[jnp.minimum(b, seqs - 1)] // size
        return jnp.where(last, b + 1, b), jnp.where(last, 0, j + 1)

    def rows_of(b):
        return pl.ds(jnp.minimum(b, seqs - 1), heads, stride=seqs)

    def copy(b, j, slot):
        return pltpu.make_async_copy(kv_hbm.at[b, :, pl.ds(pl.multiple_of(j * size, size), size)], bufs.at[slot], sems.at[slot])

    def scores(b, slot):
        q = jnp.concatenate([q_buf[n, rows_of(b), :][:, 0:hi - lo] for n, (lo, hi) in enumerate(lanes)], axis=1).astype(BF16)
        return jnp.dot(q, bufs[slot], preferred_element_type=F32)

    zero = jnp.int32(0)
    items = [(zero, zero)]
    for n in range(depth - 2):
        copy(*items[n], n).start()
        items.append(advance(*items[n]))
    copy(*items[0], 0).wait()
    copy(*items[1], 1).wait()
    s_a, s_b = scores(items[0][0], 0), scores(items[1][0], 1)
    pos = lax.broadcasted_iota(jnp.int32, (heads, size), 1)

    def absorb(b, j, slot, s, m, l, acc):
        live = b < seqs
        limit = jnp.where(live, lens_ref[jnp.minimum(b, seqs - 1)] - j * size, -1)
        s2 = jnp.where(pos <= limit, s * scale2, -jnp.inf)
        m_old = jnp.where(jnp.logical_and(live, j == 0), -jnp.inf, m)
        m_new = jnp.maximum(m_old, jnp.max(s2, axis=1, keepdims=True))
        alpha = jnp.exp2(m_old - m_new)
        p = [jnp.exp2(s2[:, k:k + 128] - m_new) for k in range(0, size, 128)]
        l_new = l * alpha + functools.reduce(jnp.add, p)
        p = jnp.concatenate([x.astype(BF16) for x in p], axis=1)
        pv = lax.dot_general(p, bufs[slot, 0:lat, :], NT, preferred_element_type=F32)
        acc = [a * alpha + pv[:, n * 128:(n + 1) * 128] for n, a in enumerate(acc)]
        for n, a in enumerate(acc):
            o_ref[n, rows_of(b), :] = a
        m_out[rows_of(b), :] = m_new
        l_out[rows_of(b), :] = l_new
        return m_new, l_new, acc

    def body(i, carry):
        (ba, ja), (bb, jb), (bc, jc), (bd, jd), (be, je), s_a, s_b, m, l, acc = carry
        t = 2 * i

        def fetch(b, j, n):
            @pl.when(n < total)
            def _():
                copy(b, j, lax.rem(n, depth)).start()

        def arrive(b, j, n):
            @pl.when(n < total)
            def _():
                copy(b, j, lax.rem(n, depth)).wait()

        bf, jf = advance(be, je)
        fetch(be, je, t + depth - 2)
        fetch(bf, jf, t + depth - 1)
        arrive(bc, jc, t + 2)
        arrive(bd, jd, t + 3)
        n_a = scores(bc, lax.rem(t + 2, depth))
        n_b = scores(bd, lax.rem(t + 3, depth))
        m, l, acc = absorb(ba, ja, lax.rem(t, depth), s_a, m, l, acc)
        m, l, acc = absorb(bb, jb, lax.rem(t + 1, depth), s_b, m, l, acc)
        bg, jg = advance(bd, jd)
        bh, jh = advance(bg, jg)
        return (bc, jc), (bd, jd), (bg, jg), (bh, jh), advance(bf, jf), n_a, n_b, m, l, acc

    third = advance(*items[1])
    stat = jnp.zeros((heads, 128), F32)
    lax.fori_loop(0, (total + 1) // 2, body, (items[0], items[1], third, advance(*third), items[-1], s_a, s_b, stat, stat, [stat] * (lat // 128)))


def suffix_part(q_rows, kv_suffix, seq_lens, heads, scale2, lat):
    rows, width = q_rows.shape
    seqs, _, slots = kv_suffix.shape
    size, depth = 512, 12
    stat = jax.ShapeDtypeStruct((rows, 128), F32)
    return pl.pallas_call(
        functools.partial(suffix_kernel, scale2, lat, heads),
        out_shape=[jax.ShapeDtypeStruct((lat // 128, rows, 128), F32), stat, stat],
        in_specs=[SMEM, VMEM, HBM],
        out_specs=[VMEM, VMEM, VMEM],
        scratch_shapes=[pltpu.VMEM((-(-width // 128), rows, 128), F32), pltpu.VMEM((depth, width, size), BF16), pltpu.SemaphoreType.DMA((depth,))],
        compiler_params=pltpu.CompilerParams(vmem_limit_bytes=32 * 2**20),
        cost_estimate=pl.CostEstimate(flops=2 * seqs * slots * 256 * 768, bytes_accessed=seqs * slots * width * 2, transcendentals=seqs * slots * heads),
        name='suffix',
    )(seq_lens, q_rows, kv_suffix)


def stats_of(ref, size):
    both = ref[size:size + 8, 0:size].T
    return both[:, 0:1], both[:, 1:2]


def merge_kernel(x_ref, y_ref, o_ref, offset):
    rows, half = x_ref.shape[0] - 8, y_ref.shape[0] - 8
    cut = slice(offset, offset + half)
    rest = slice(half - offset, 2 * half - offset)
    m_x, m_y = x_ref[rows:rows + 1, cut], y_ref[half:half + 1, 0:half]
    l_x, l_y = x_ref[rows + 1:rows + 2, cut], y_ref[half + 1:half + 2, 0:half]
    m_all = jnp.maximum(m_x, m_y)
    w_x, w_y = jnp.exp2(m_x - m_all), jnp.exp2(m_y - m_all)
    o_ref[rows:rows + 1, cut] = m_all
    o_ref[rows + 1:rows + 2, cut] = l_x * w_x + l_y * w_y
    o_ref[rows:rows + 2, rest] = x_ref[rows:rows + 2, rest]
    c_x = jnp.broadcast_to(w_x, (8, half)).T[:, 0:1]
    c_y = jnp.broadcast_to(w_y, (8, half)).T[:, 0:1]
    o_ref[cut, :] = x_ref[cut, :] * c_x + y_ref[0:half, :] * c_y
    o_ref[rest, :] = x_ref[rest, :]


def merge_parts(x, y, offset, name):
    return pl.pallas_call(
        functools.partial(merge_kernel, offset=offset),
        out_shape=jax.ShapeDtypeStruct(x.shape, F32),
        in_specs=[VMEM, VMEM],
        out_specs=VMEM,
        compiler_params=pltpu.CompilerParams(vmem_limit_bytes=8 * 2**20),
        cost_estimate=pl.CostEstimate(flops=4 * x.size, bytes_accessed=12 * x.size, transcendentals=0),
        name=name,
    )(x, y)


def output_kernel(hid_ref, os_ref, ms_ref, ls_ref, *refs):
    parts, (uv_ref, wo_ref, out_ref, v_buf) = refs[:3], refs[3:]
    rows, heads = hid_ref.shape[0], uv_ref.shape[0]
    lat, width = uv_ref.shape[1], uv_ref.shape[2]
    flat = rows * heads
    stats = [stats_of(ref, flat) for ref in parts]
    for h in range(heads):
        cut = slice(h * rows, (h + 1) * rows)
        m_s, l_s = ms_ref[cut, 0:1], jnp.sum(ls_ref[cut, :], axis=1, keepdims=True)
        ms = [m_s] + [m[cut] for m, _ in stats]
        ls = [l_s] + [l[cut] for _, l in stats]
        m_all = functools.reduce(jnp.maximum, ms)
        ws = [jnp.exp2(m - m_all) for m in ms]
        l_all = functools.reduce(jnp.add, [l * w for l, w in zip(ls, ws)])
        o_s = jnp.concatenate([os_ref[n, cut, :] for n in range(lat // 128)], axis=1)
        o_all = o_s * ws[0]
        for ref, w in zip(parts, ws[1:]):
            o_all = o_all + ref[cut, :] * w
        o_h = (o_all / l_all).astype(BF16)
        v_buf[:, h * width:(h + 1) * width] = jnp.dot(o_h, uv_ref[h], preferred_element_type=F32).astype(BF16)
    proj = jnp.dot(v_buf[...], wo_ref[...], preferred_element_type=F32)
    out_ref[...] = (hid_ref[...].astype(F32) + proj).astype(BF16)


def output_part(hidden, suffix, parts, w_uv, w_o):
    rows = hidden.shape[0]
    heads, lat, val = w_uv.shape
    return pl.pallas_call(
        output_kernel,
        out_shape=jax.ShapeDtypeStruct(hidden.shape, BF16),
        in_specs=[VMEM] * 9,
        out_specs=VMEM,
        scratch_shapes=[pltpu.VMEM((rows, heads * val), BF16)],
        compiler_params=pltpu.CompilerParams(vmem_limit_bytes=24 * 2**20),
        cost_estimate=pl.CostEstimate(flops=2 * rows * heads * val * (lat + hidden.shape[1]), bytes_accessed=2 * (w_uv.size + w_o.size), transcendentals=0),
        name='output',
    )(hidden, *suffix, *parts, w_uv, w_o)


def solution(mesh):
    group = mesh.shape['ctx']
    chips = group // CORES
    rows_spec = P(('dp', 'ctx'), None)
    whole_spec = P()

    def local_step(hidden, w_q, w_uk, w_uv, w_o, kv_prefix, kv_suffix, seq_lens):
        rows = hidden.shape[0]
        heads, nope, lat = w_uk.shape
        head_w = w_q.shape[1] // heads
        rope = head_w - nope
        prefix_len = kv_prefix.shape[0] * group
        scale2 = head_w ** -0.5 * LOG2E
        kv_prefix = kv_prefix.T
        kv_suffix = kv_suffix.transpose(0, 2, 1)
        cs = rope_table(prefix_len + seq_lens, rope // 2)
        q_all, keys = gather_queries(hidden, cs, w_q, w_uk, kv_prefix, chips)
        q_all = q_all.reshape(chips, heads * rows, -1)

        def send(value, hop):
            return lax.ppermute(value, 'ctx', [(j, (j + hop * CORES) % group) for j in range(group)])

        def after(value, *earlier):
            return lax.optimization_barrier((value,) + earlier)[0]

        def part(query, pieces, name):
            return prefix_part(query, keys, scale2, lat, pieces, name)

        far_a, far_b = part(q_all[2], 2, 'prefix_far')
        got_a = send(far_a, 1)
        got_b = send(far_b, -1)
        up, = part(after(q_all[1], far_a, far_b), 1, 'prefix_up')
        down, = part(after(q_all[3], up), 1, 'prefix_down')
        up = merge_parts(after(up, down), got_a, 0, 'merge_up')
        in_up = send(up, 1)
        down = merge_parts(after(down, up), got_b, heads * rows // 2, 'merge_down')
        in_down = send(down, -1)
        own, = part(after(q_all[0], down), 1, 'prefix_own')
        suffix = suffix_part(after(q_all[0], own), kv_suffix, seq_lens, heads, scale2, lat)
        return output_part(hidden, suffix, (own, in_up, in_down), w_uv, w_o)

    return jax.shard_map(local_step, mesh=mesh, in_specs=(rows_spec, whole_spec, whole_spec, whole_spec, whole_spec, rows_spec, P(('dp', 'ctx'), None, None), P(('dp', 'ctx'))), out_specs=rows_spec, check_vma=False)
```

```python
import functools
import math
import jax
import jax.numpy as jnp
from jax import lax
from jax.experimental import pallas as pl
from jax.experimental.pallas import tpu as pltpu
from jax.sharding import PartitionSpec as P

ROPE_BASE = 10000
LOG2E = math.log2(math.e)
CORES = 2
F32 = jnp.float32
BF16 = jnp.bfloat16
HBM = pl.BlockSpec(memory_space=pltpu.HBM)
VMEM = pl.BlockSpec(memory_space=pltpu.VMEM)
SMEM = pl.BlockSpec(memory_space=pltpu.SMEM)
NT = (((1,), (1,)), ((), ()))


def rope_table(positions, half_dim):
    inv_freq = jnp.exp(jnp.arange(half_dim, dtype=F32) * (-math.log(ROPE_BASE) / half_dim))
    angle = positions.astype(F32)[:, None] * inv_freq
    cos_part = jnp.cos(angle)
    sin_part = jnp.sin(angle)
    return jnp.concatenate([cos_part, cos_part, sin_part, sin_part], axis=-1)


def prefix_part(scale2, lat, q_ref, k_ref, outs, work, hook=None):
    s_ref, p_ref, acc_ref, a_ref, m_ref, l_ref = work
    rows, sub = q_ref.shape[0], s_ref.shape[2]
    count = k_ref.shape[1] // sub
    chunk = 64
    m_ref[...] = jnp.full_like(m_ref, -jnp.inf)
    l_ref[...] = jnp.zeros_like(l_ref)
    acc_ref[...] = jnp.zeros_like(acc_ref)

    def keys(n):
        return pl.ds(pl.multiple_of(n * sub, sub), sub)

    def scores(n, slot):
        s_ref[slot] = jnp.dot(q_ref[...], k_ref[:, keys(n)], preferred_element_type=F32)

    def absorb(n, slot):
        for r in range(0, rows, chunk):
            cut = slice(r, r + chunk)
            s = s_ref[slot, cut, :]
            m_old = m_ref[cut, :]
            m_new = jnp.maximum(m_old, jnp.max(s, axis=1, keepdims=True) * scale2)
            alpha = jnp.exp2(m_old - m_new)
            l_new = l_ref[cut, :] * alpha
            for k in range(0, sub, 128):
                p = jnp.exp2(s[:, k:k + 128] * scale2 - m_new)
                l_new = l_new + p
                p_ref[slot, cut, k:k + 128] = p.astype(BF16)
            l_ref[cut, :] = l_new
            m_ref[cut, :] = m_new
            a_ref[cut, :] = alpha
        pv = lax.dot_general(p_ref[slot], k_ref[0:lat, keys(n)], NT, preferred_element_type=F32)
        alpha = a_ref[...]
        for k in range(0, lat, 128):
            acc_ref[:, k:k + 128] = acc_ref[:, k:k + 128] * alpha + pv[:, k:k + 128]

    scores(0, 0)
    if hook is not None:
        hook()

    def pair(i, carry):
        scores(2 * i + 1, 1)
        absorb(2 * i, 0)
        scores(2 * i + 2, 0)
        absorb(2 * i + 1, 1)
        return carry

    lax.fori_loop(0, count // 2 - 1, pair, 0)
    scores(count - 1, 1)
    absorb(count - 2, 0)
    absorb(count - 1, 1)
    m_t = m_ref[...].T[0:1]
    l_t = jnp.broadcast_to(jnp.sum(l_ref[...], axis=1, keepdims=True), (rows, 128)).T[0:1]
    size = rows // len(outs)
    for k, ref in enumerate(outs):
        cut = slice(k * size, (k + 1) * size)
        ref[0:size, :] = acc_ref[cut, :]
        ref[size:size + 1, 0:size] = m_t[:, cut]
        ref[size + 1:size + 2, 0:size] = l_t[:, cut]


def merge_into(x_ref, y_ref, offset):
    rows, half = x_ref.shape[0] - 8, y_ref.shape[0] - 8
    cut = slice(offset, offset + half)
    m_x, m_y = x_ref[rows:rows + 1, cut], y_ref[half:half + 1, 0:half]
    l_x, l_y = x_ref[rows + 1:rows + 2, cut], y_ref[half + 1:half + 2, 0:half]
    m_all = jnp.maximum(m_x, m_y)
    w_x, w_y = jnp.exp2(m_x - m_all), jnp.exp2(m_y - m_all)
    x_ref[rows:rows + 1, cut] = m_all
    x_ref[rows + 1:rows + 2, cut] = l_x * w_x + l_y * w_y
    c_x = jnp.broadcast_to(w_x, (8, half)).T[:, 0:1]
    c_y = jnp.broadcast_to(w_y, (8, half)).T[:, 0:1]
    x_ref[cut, :] = x_ref[cut, :] * c_x + y_ref[0:half, :] * c_y


def prefix_kernel(chips, scale2, hid_ref, cs_ref, wq_hbm, wuk_hbm, kv_hbm, q_out, own_out, up_out, down_out,
                  hid_all, cs_all, wq_buf, wuk_buf, k_ref, q_buf, res, far, got,
                  s_ref, p_ref, acc_ref, a_ref, m_ref, l_ref,
                  wq_sem, wuk_sem, kv_sem, out_sem, hid_send, hid_recv, cs_send, cs_recv, kv_send, kv_recv, far_send, far_recv):
    me = lax.axis_index('ctx')
    chip, core = me // CORES, me % CORES
    steps, _, wide = wq_buf.shape
    rows = hid_ref.shape[0]
    heads, nope, lat = wuk_buf.shape
    rope = q_buf.shape[2] - lat
    head_w = nope + rope
    keys = kv_hbm.shape[1]
    per = wide // head_w
    work = (s_ref, p_ref, acc_ref, a_ref, m_ref, l_ref)

    def weight_copy(i):
        return pltpu.make_async_copy(wq_hbm.at[:, pl.ds(i * wide, wide)], wq_buf.at[i], wq_sem.at[i])

    def remote(src, dst, send, recv, dev):
        return pltpu.make_async_remote_copy(src, dst, send, recv, device_id={'ctx': dev}, device_id_type=pl.DeviceIdType.MESH)

    weight_copy(0).start()
    uk_copy = pltpu.make_async_copy(wuk_hbm, wuk_buf, wuk_sem)
    uk_copy.start()
    for i in range(1, steps):
        weight_copy(i).start()
    own_copy = pltpu.make_async_copy(kv_hbm, k_ref.at[:, pl.ds(0, keys)], kv_sem)
    own_copy.start()
    partner = chip * CORES + (1 - core)
    peers = [((chip + chips - r) % chips) * CORES + core for r in range(1, chips)]
    barrier = pltpu.get_barrier_semaphore()
    for dev in [partner] + peers:
        pl.semaphore_signal(barrier, inc=1, device_id={'ctx': dev}, device_id_type=pl.DeviceIdType.MESH)
    pl.semaphore_wait(barrier, chips)
    copies = []
    for r in range(1, chips):
        copies.append(remote(hid_ref, hid_all.at[r - 1], hid_send.at[r - 1], hid_recv.at[r - 1], peers[r - 1]))
        copies.append(remote(cs_ref, cs_all.at[r - 1], cs_send.at[r - 1], cs_recv.at[r - 1], peers[r - 1]))
    kv_copy = remote(kv_hbm, k_ref.at[:, pl.ds(keys, keys)], kv_send, kv_recv, partner)
    kv_copy.start()
    for c in copies:
        c.start()

    def queries(x, cs, first, own):
        cos, sin = cs[:, :rope], cs[:, rope:]
        for i in range(steps):
            if own:
                weight_copy(i).wait()
            qa = jnp.dot(x, wq_buf[i], preferred_element_type=F32).astype(BF16)
            if own and i == 0:
                uk_copy.wait()
            for k in range(per):
                h = i * per + k
                q_lat = jnp.dot(qa[:, k * head_w:k * head_w + nope], wuk_buf[h], preferred_element_type=F32).astype(BF16)
                pe = qa[:, k * head_w + nope:(k + 1) * head_w].astype(F32)
                turned = jnp.concatenate([-pe[:, rope // 2:], pe[:, :rope // 2]], axis=1)
                pe = (pe * cos + turned * sin).astype(BF16)
                for r in range(x.shape[0] // rows):
                    q_buf[first + r, h * rows:(h + 1) * rows, 0:lat] = q_lat[r * rows:(r + 1) * rows]
                    q_buf[first + r, h * rows:(h + 1) * rows, lat:lat + rope] = pe[r * rows:(r + 1) * rows]

    queries(hid_ref[...], cs_ref[...], 0, True)
    q_copy = pltpu.make_async_copy(q_buf.at[0], q_out, out_sem.at[0])
    own_copy.wait()
    kv_copy.wait()
    prefix_part(scale2, lat, q_buf.at[0], k_ref, [res.at[0]], work, q_copy.start)
    for c in copies:
        c.wait()
    queries(hid_all[...].reshape((chips - 1) * rows, hid_ref.shape[1]), cs_all[...].reshape((chips - 1) * rows, 2 * rope), 1, False)
    own_done = pltpu.make_async_copy(res.at[0], own_out, out_sem.at[1])
    prefix_part(scale2, lat, q_buf.at[2], k_ref, [far.at[0], far.at[1]], work, own_done.start)
    sends = [remote(far.at[n], got.at[n], far_send.at[n], far_recv.at[n], dev) for n, dev in enumerate((peers[2], peers[0]))]

    def send_far():
        for c in sends:
            c.start()

    prefix_part(scale2, lat, q_buf.at[1], k_ref, [res.at[1]], work, send_far)
    prefix_part(scale2, lat, q_buf.at[3], k_ref, [res.at[2]], work)
    for c in sends:
        c.wait()
    merge_into(res.at[1], got.at[0], 0)
    merge_into(res.at[2], got.at[1], heads * rows // 2)
    last = [pltpu.make_async_copy(res.at[1], up_out, out_sem.at[2]), pltpu.make_async_copy(res.at[2], down_out, out_sem.at[3])]
    for c in last:
        c.start()
    for c in [q_copy, own_done] + last:
        c.wait()


def prefix_parts(hidden, cs, w_q, w_uk, kv_prefix, scale2, chips):
    rows, depth = hidden.shape
    heads, nope, lat = w_uk.shape
    rope = w_q.shape[1] // heads - nope
    steps, sub = 4, 512
    wide = w_q.shape[1] // steps
    flat = heads * rows
    keys = CORES * kv_prefix.shape[1]
    others = chips - 1
    full, half = (flat + 8, lat), (flat // 2 + 8, lat)
    dma = pltpu.SemaphoreType.DMA
    return pl.pallas_call(
        functools.partial(prefix_kernel, chips, scale2),
        out_shape=[jax.ShapeDtypeStruct((flat, lat + rope), BF16)] + [jax.ShapeDtypeStruct(full, F32)] * 3,
        in_specs=[VMEM, VMEM, HBM, HBM, HBM],
        out_specs=[HBM] * 4,
        scratch_shapes=[
            pltpu.VMEM((others, rows, depth), BF16), pltpu.VMEM((others, rows, 2 * rope), F32),
            pltpu.VMEM((steps, depth, wide), BF16), pltpu.VMEM(w_uk.shape, BF16),
            pltpu.VMEM((kv_prefix.shape[0], keys), BF16), pltpu.VMEM((chips, flat, lat + rope), BF16),
            pltpu.VMEM((3,) + full, F32), pltpu.VMEM((2,) + half, F32), pltpu.VMEM((2,) + half, F32),
            pltpu.VMEM((2, flat, sub), F32), pltpu.VMEM((2, flat, sub), BF16), pltpu.VMEM((flat, lat), F32)]
            + [pltpu.VMEM((flat, 128), F32)] * 3
            + [dma((steps,)), dma, dma, dma((4,)), dma((others,)), dma((others,)), dma((others,)), dma((others,)), dma, dma, dma((2,)), dma((2,))],
        compiler_params=pltpu.CompilerParams(collective_id=0, has_side_effects=True, vmem_limit_bytes=60 * 2**20),
        cost_estimate=pl.CostEstimate(flops=2 * chips * flat * keys * (768 + lat), bytes_accessed=2 * w_q.size, transcendentals=chips * flat * keys),
        name='prefix',
    )(hidden, cs, w_q, w_uk, kv_prefix)


def suffix_kernel(scale2, lat, heads, lens_ref, q_ref, kv_hbm, o_ref, m_out, l_out, q_buf, bufs, sems):
    seqs = q_ref.shape[0] // heads
    width = q_ref.shape[1]
    depth, size = bufs.shape[0], bufs.shape[2]
    lanes = [(k, min(k + 128, width)) for k in range(0, width, 128)]
    for n, (lo, hi) in enumerate(lanes):
        q_buf[n, :, 0:hi - lo] = q_ref[:, lo:hi].astype(F32)

    total = lax.fori_loop(0, seqs, lambda b, n: n + lens_ref[b] // size + 1, 0)

    def advance(b, j):
        last = j >= lens_ref[jnp.minimum(b, seqs - 1)] // size
        return jnp.where(last, b + 1, b), jnp.where(last, 0, j + 1)

    def rows_of(b):
        return pl.ds(jnp.minimum(b, seqs - 1), heads, stride=seqs)

    def copy(b, j, slot):
        return pltpu.make_async_copy(kv_hbm.at[b, :, pl.ds(pl.multiple_of(j * size, size), size)], bufs.at[slot], sems.at[slot])

    def scores(b, slot):
        q = jnp.concatenate([q_buf[n, rows_of(b), :][:, 0:hi - lo] for n, (lo, hi) in enumerate(lanes)], axis=1).astype(BF16)
        return jnp.dot(q, bufs[slot], preferred_element_type=F32)

    zero = jnp.int32(0)
    items = [(zero, zero)]
    for n in range(depth - 2):
        copy(*items[n], n).start()
        items.append(advance(*items[n]))
    copy(*items[0], 0).wait()
    copy(*items[1], 1).wait()
    s_a, s_b = scores(items[0][0], 0), scores(items[1][0], 1)
    pos = lax.broadcasted_iota(jnp.int32, (heads, size), 1)

    def absorb(b, j, slot, s, m, l, acc):
        live = b < seqs
        limit = jnp.where(live, lens_ref[jnp.minimum(b, seqs - 1)] - j * size, -1)
        s2 = jnp.where(pos <= limit, s * scale2, -jnp.inf)
        m_old = jnp.where(jnp.logical_and(live, j == 0), -jnp.inf, m)
        m_new = jnp.maximum(m_old, jnp.max(s2, axis=1, keepdims=True))
        alpha = jnp.exp2(m_old - m_new)
        p = [jnp.exp2(s2[:, k:k + 128] - m_new) for k in range(0, size, 128)]
        l_new = l * alpha + functools.reduce(jnp.add, p)
        p = jnp.concatenate([x.astype(BF16) for x in p], axis=1)
        pv = lax.dot_general(p, bufs[slot, 0:lat, :], NT, preferred_element_type=F32)
        acc = [a * alpha + pv[:, n * 128:(n + 1) * 128] for n, a in enumerate(acc)]
        for n, a in enumerate(acc):
            o_ref[n, rows_of(b), :] = a
        m_out[rows_of(b), :] = m_new
        l_out[rows_of(b), :] = l_new
        return m_new, l_new, acc

    def body(i, carry):
        (ba, ja), (bb, jb), (bc, jc), (bd, jd), (be, je), s_a, s_b, m, l, acc = carry
        t = 2 * i

        def fetch(b, j, n):
            @pl.when(n < total)
            def _():
                copy(b, j, lax.rem(n, depth)).start()

        def arrive(b, j, n):
            @pl.when(n < total)
            def _():
                copy(b, j, lax.rem(n, depth)).wait()

        bf, jf = advance(be, je)
        fetch(be, je, t + depth - 2)
        fetch(bf, jf, t + depth - 1)
        arrive(bc, jc, t + 2)
        arrive(bd, jd, t + 3)
        n_a = scores(bc, lax.rem(t + 2, depth))
        n_b = scores(bd, lax.rem(t + 3, depth))
        m, l, acc = absorb(ba, ja, lax.rem(t, depth), s_a, m, l, acc)
        m, l, acc = absorb(bb, jb, lax.rem(t + 1, depth), s_b, m, l, acc)
        bg, jg = advance(bd, jd)
        bh, jh = advance(bg, jg)
        return (bc, jc), (bd, jd), (bg, jg), (bh, jh), advance(bf, jf), n_a, n_b, m, l, acc

    third = advance(*items[1])
    stat = jnp.zeros((heads, 128), F32)
    lax.fori_loop(0, (total + 1) // 2, body, (items[0], items[1], third, advance(*third), items[-1], s_a, s_b, stat, stat, [stat] * (lat // 128)))


def suffix_part(q_rows, kv_suffix, seq_lens, heads, scale2, lat):
    rows, width = q_rows.shape
    seqs, _, slots = kv_suffix.shape
    size, depth = 512, 12
    stat = jax.ShapeDtypeStruct((rows, 128), F32)
    return pl.pallas_call(
        functools.partial(suffix_kernel, scale2, lat, heads),
        out_shape=[jax.ShapeDtypeStruct((lat // 128, rows, 128), F32), stat, stat],
        in_specs=[SMEM, VMEM, HBM],
        out_specs=[VMEM, VMEM, VMEM],
        scratch_shapes=[pltpu.VMEM((-(-width // 128), rows, 128), F32), pltpu.VMEM((depth, width, size), BF16), pltpu.SemaphoreType.DMA((depth,))],
        compiler_params=pltpu.CompilerParams(vmem_limit_bytes=32 * 2**20),
        cost_estimate=pl.CostEstimate(flops=2 * seqs * slots * 256 * 768, bytes_accessed=seqs * slots * width * 2, transcendentals=seqs * slots * heads),
        name='suffix',
    )(seq_lens, q_rows, kv_suffix)


def stats_of(ref, size):
    both = ref[size:size + 8, 0:size].T
    return both[:, 0:1], both[:, 1:2]


def output_kernel(hid_ref, os_ref, ms_ref, ls_ref, *refs):
    parts, (uv_ref, wo_ref, out_ref, v_buf) = refs[:3], refs[3:]
    rows, heads = hid_ref.shape[0], uv_ref.shape[0]
    lat, width = uv_ref.shape[1], uv_ref.shape[2]
    flat = rows * heads
    stats = [stats_of(ref, flat) for ref in parts]
    for h in range(heads):
        cut = slice(h * rows, (h + 1) * rows)
        m_s, l_s = ms_ref[cut, 0:1], jnp.sum(ls_ref[cut, :], axis=1, keepdims=True)
        ms = [m_s] + [m[cut] for m, _ in stats]
        ls = [l_s] + [l[cut] for _, l in stats]
        m_all = functools.reduce(jnp.maximum, ms)
        ws = [jnp.exp2(m - m_all) for m in ms]
        l_all = functools.reduce(jnp.add, [l * w for l, w in zip(ls, ws)])
        o_s = jnp.concatenate([os_ref[n, cut, :] for n in range(lat // 128)], axis=1)
        o_all = o_s * ws[0]
        for ref, w in zip(parts, ws[1:]):
            o_all = o_all + ref[cut, :] * w
        o_h = (o_all / l_all).astype(BF16)
        v_buf[:, h * width:(h + 1) * width] = jnp.dot(o_h, uv_ref[h], preferred_element_type=F32).astype(BF16)
    proj = jnp.dot(v_buf[...], wo_ref[...], preferred_element_type=F32)
    out_ref[...] = (hid_ref[...].astype(F32) + proj).astype(BF16)


def output_part(hidden, suffix, parts, w_uv, w_o):
    rows = hidden.shape[0]
    heads, lat, val = w_uv.shape
    return pl.pallas_call(
        output_kernel,
        out_shape=jax.ShapeDtypeStruct(hidden.shape, BF16),
        in_specs=[VMEM] * 9,
        out_specs=VMEM,
        scratch_shapes=[pltpu.VMEM((rows, heads * val), BF16)],
        compiler_params=pltpu.CompilerParams(vmem_limit_bytes=24 * 2**20),
        cost_estimate=pl.CostEstimate(flops=2 * rows * heads * val * (lat + hidden.shape[1]), bytes_accessed=2 * (w_uv.size + w_o.size), transcendentals=0),
        name='output',
    )(hidden, *suffix, *parts, w_uv, w_o)


def solution(mesh):
    group = mesh.shape['ctx']
    chips = group // CORES
    rows_spec = P(('dp', 'ctx'), None)
    whole_spec = P()

    def local_step(hidden, w_q, w_uk, w_uv, w_o, kv_prefix, kv_suffix, seq_lens):
        rows = hidden.shape[0]
        heads, nope, lat = w_uk.shape
        head_w = w_q.shape[1] // heads
        rope = head_w - nope
        prefix_len = kv_prefix.shape[0] * group
        scale2 = head_w ** -0.5 * LOG2E
        kv_prefix = kv_prefix.T
        kv_suffix = kv_suffix.transpose(0, 2, 1)
        cs = rope_table(prefix_len + seq_lens, rope // 2)
        query, own, up, down = prefix_parts(hidden, cs, w_q, w_uk, kv_prefix, scale2, chips)

        def send(value, hop):
            return lax.ppermute(value, 'ctx', [(j, (j + hop * CORES) % group) for j in range(group)])

        in_up, in_down = send(up, 1), send(down, -1)
        suffix = suffix_part(query, kv_suffix, seq_lens, heads, scale2, lat)
        return output_part(hidden, suffix, (own, in_up, in_down), w_uv, w_o)

    return jax.shard_map(local_step, mesh=mesh, in_specs=(rows_spec, whole_spec, whole_spec, whole_spec, whole_spec, rows_spec, P(('dp', 'ctx'), None, None), P(('dp', 'ctx'))), out_specs=rows_spec, check_vma=False)
```

```python
import functools
import math
import jax
import jax.numpy as jnp
from jax import lax
from jax.experimental import pallas as pl
from jax.experimental.pallas import tpu as pltpu
from jax.sharding import PartitionSpec as P

ROPE_BASE = 10000
LOG2E = math.log2(math.e)
CORES = 2
F32 = jnp.float32
BF16 = jnp.bfloat16
HBM = pl.BlockSpec(memory_space=pltpu.HBM)
VMEM = pl.BlockSpec(memory_space=pltpu.VMEM)
SMEM = pl.BlockSpec(memory_space=pltpu.SMEM)
NT = (((1,), (1,)), ((), ()))


def rope_table(positions, half_dim):
    lane = jnp.arange(4 * half_dim)
    inv_freq = jnp.exp((lane % half_dim).astype(F32) * (-math.log(ROPE_BASE) / half_dim))
    angle = positions.astype(F32)[:, None] * inv_freq
    return jnp.where(lane < 2 * half_dim, jnp.cos(angle), jnp.sin(angle))


def prefix_part(scale2, lat, q_ref, k_ref, outs, work, hook=None, loaded=False, next_ref=None):
    s_ref, p_ref, acc_ref, a_ref, m_ref, l_ref = work
    rows, sub = q_ref.shape[0], s_ref.shape[2]
    count = k_ref.shape[1] // sub
    chunk = 64
    m_ref[...] = jnp.full_like(m_ref, -jnp.inf)
    l_ref[...] = jnp.zeros_like(l_ref)
    acc_ref[...] = jnp.zeros_like(acc_ref)

    def keys(n):
        return pl.ds(pl.multiple_of(n * sub, sub), sub)

    def scores(n, slot, ref=q_ref):
        s_ref[slot] = jnp.dot(ref[...], k_ref[:, keys(n)], preferred_element_type=F32)

    def absorb(n, slot):
        for r in range(0, rows, chunk):
            cut = slice(r, r + chunk)
            s = s_ref[slot, cut, :]
            m_old = m_ref[cut, :]
            m_new = jnp.maximum(m_old, jnp.max(s, axis=1, keepdims=True) * scale2)
            alpha = jnp.exp2(m_old - m_new)
            l_new = l_ref[cut, :] * alpha
            for k in range(0, sub, 128):
                p = jnp.exp2(s[:, k:k + 128] * scale2 - m_new)
                l_new = l_new + p
                p_ref[slot, cut, k:k + 128] = p.astype(BF16)
            l_ref[cut, :] = l_new
            m_ref[cut, :] = m_new
            a_ref[cut, :] = alpha
        pv = lax.dot_general(p_ref[slot], k_ref[0:lat, keys(n)], NT, preferred_element_type=F32)
        alpha = a_ref[...]
        for k in range(0, lat, 128):
            acc_ref[:, k:k + 128] = acc_ref[:, k:k + 128] * alpha + pv[:, k:k + 128]

    if not loaded:
        scores(0, 0)
    if hook is not None:
        hook()

    def pair(i, carry):
        scores(2 * i + 1, 1)
        absorb(2 * i, 0)
        scores(2 * i + 2, 0)
        absorb(2 * i + 1, 1)
        return carry

    lax.fori_loop(0, count // 2 - 1, pair, 0)
    scores(count - 1, 1)
    absorb(count - 2, 0)
    if next_ref is not None:
        scores(0, 0, next_ref)
    absorb(count - 1, 1)
    m_t = m_ref[...].T[0:1]
    l_t = jnp.broadcast_to(jnp.sum(l_ref[...], axis=1, keepdims=True), (rows, 128)).T[0:1]
    size = rows // len(outs)
    for k, ref in enumerate(outs):
        cut = slice(k * size, (k + 1) * size)
        ref[0:size, :] = acc_ref[cut, :]
        ref[size:size + 1, 0:size] = m_t[:, cut]
        ref[size + 1:size + 2, 0:size] = l_t[:, cut]


def merge_into(x_ref, y_ref, offset):
    rows, half = x_ref.shape[0] - 8, y_ref.shape[0] - 8
    cut = slice(offset, offset + half)
    m_x, m_y = x_ref[rows:rows + 1, cut], y_ref[half:half + 1, 0:half]
    l_x, l_y = x_ref[rows + 1:rows + 2, cut], y_ref[half + 1:half + 2, 0:half]
    m_all = jnp.maximum(m_x, m_y)
    w_x, w_y = jnp.exp2(m_x - m_all), jnp.exp2(m_y - m_all)
    x_ref[rows:rows + 1, cut] = m_all
    x_ref[rows + 1:rows + 2, cut] = l_x * w_x + l_y * w_y
    c_x = jnp.broadcast_to(w_x, (8, half)).T[:, 0:1]
    c_y = jnp.broadcast_to(w_y, (8, half)).T[:, 0:1]
    x_ref[cut, :] = x_ref[cut, :] * c_x + y_ref[0:half, :] * c_y


def prefix_kernel(chips, scale2, hid_ref, cs_ref, wq_hbm, wuk_hbm, kv_hbm, q_out, own_out, up_out, down_out,
                  hid_all, cs_all, wq_buf, wuk_buf, k_ref, q_buf, res, far, got,
                  s_ref, p_ref, acc_ref, a_ref, m_ref, l_ref,
                  wq_sem, wuk_sem, kv_sem, out_sem, hid_send, hid_recv, cs_send, cs_recv, kv_send, kv_recv, far_send, far_recv):
    me = lax.axis_index('ctx')
    chip, core = me // CORES, me % CORES
    steps, _, wide = wq_buf.shape
    rows = hid_ref.shape[0]
    heads, nope, lat = wuk_buf.shape
    rope = q_buf.shape[2] - lat
    head_w = nope + rope
    keys = kv_hbm.shape[1]
    per = wide // head_w
    work = (s_ref, p_ref, acc_ref, a_ref, m_ref, l_ref)

    def weight_copy(i):
        return pltpu.make_async_copy(wq_hbm.at[:, pl.ds(i * wide, wide)], wq_buf.at[i], wq_sem.at[i])

    def remote(src, dst, send, recv, dev):
        return pltpu.make_async_remote_copy(src, dst, send, recv, device_id={'ctx': dev}, device_id_type=pl.DeviceIdType.MESH)

    weight_copy(0).start()
    uk_copy = pltpu.make_async_copy(wuk_hbm, wuk_buf, wuk_sem)
    uk_copy.start()
    for i in range(1, steps):
        weight_copy(i).start()
    own_copy = pltpu.make_async_copy(kv_hbm, k_ref.at[:, pl.ds(0, keys)], kv_sem)
    own_copy.start()
    partner = chip * CORES + (1 - core)
    peers = [((chip + chips - r) % chips) * CORES + core for r in range(1, chips)]
    barrier = pltpu.get_barrier_semaphore()
    for dev in [partner] + peers:
        pl.semaphore_signal(barrier, inc=1, device_id={'ctx': dev}, device_id_type=pl.DeviceIdType.MESH)
    pl.semaphore_wait(barrier, chips)
    copies = []
    for r in range(1, chips):
        copies.append(remote(hid_ref, hid_all.at[r - 1], hid_send.at[r - 1], hid_recv.at[r - 1], peers[r - 1]))
        copies.append(remote(cs_ref, cs_all.at[r - 1], cs_send.at[r - 1], cs_recv.at[r - 1], peers[r - 1]))
    kv_copy = remote(kv_hbm, k_ref.at[:, pl.ds(keys, keys)], kv_send, kv_recv, partner)
    kv_copy.start()
    for c in copies:
        c.start()

    def queries(x, cs, first, own):
        cos, sin = cs[:, :rope], cs[:, rope:]
        for i in range(steps):
            if own:
                weight_copy(i).wait()
            qa = jnp.dot(x, wq_buf[i], preferred_element_type=F32).astype(BF16)
            if own and i == 0:
                uk_copy.wait()
            for k in range(per):
                h = i * per + k
                q_lat = jnp.dot(qa[:, k * head_w:k * head_w + nope], wuk_buf[h], preferred_element_type=F32).astype(BF16)
                pe = qa[:, k * head_w + nope:(k + 1) * head_w].astype(F32)
                turned = jnp.concatenate([-pe[:, rope // 2:], pe[:, :rope // 2]], axis=1)
                pe = (pe * cos + turned * sin).astype(BF16)
                for r in range(x.shape[0] // rows):
                    q_buf[first + r, h * rows:(h + 1) * rows, 0:lat] = q_lat[r * rows:(r + 1) * rows]
                    q_buf[first + r, h * rows:(h + 1) * rows, lat:lat + rope] = pe[r * rows:(r + 1) * rows]

    queries(hid_ref[...], cs_ref[...], 0, True)
    q_copy = pltpu.make_async_copy(q_buf.at[0], q_out, out_sem.at[0])
    own_copy.wait()
    kv_copy.wait()
    prefix_part(scale2, lat, q_buf.at[0], k_ref, [res.at[0]], work, q_copy.start)
    for c in copies:
        c.wait()
    queries(hid_all[...].reshape((chips - 1) * rows, hid_ref.shape[1]), cs_all[...].reshape((chips - 1) * rows, 2 * rope), 1, False)
    own_done = pltpu.make_async_copy(res.at[0], own_out, out_sem.at[1])
    prefix_part(scale2, lat, q_buf.at[2], k_ref, [far.at[0], far.at[1]], work, own_done.start, next_ref=q_buf.at[1])
    sends = [remote(far.at[n], got.at[n], far_send.at[n], far_recv.at[n], dev) for n, dev in enumerate((peers[2], peers[0]))]

    def send_far():
        for c in sends:
            c.start()

    prefix_part(scale2, lat, q_buf.at[1], k_ref, [res.at[1]], work, send_far, loaded=True, next_ref=q_buf.at[3])
    prefix_part(scale2, lat, q_buf.at[3], k_ref, [res.at[2]], work, loaded=True)
    for c in sends:
        c.wait()
    merge_into(res.at[1], got.at[0], 0)
    merge_into(res.at[2], got.at[1], heads * rows // 2)
    last = [pltpu.make_async_copy(res.at[1], up_out, out_sem.at[2]), pltpu.make_async_copy(res.at[2], down_out, out_sem.at[3])]
    for c in last:
        c.start()
    for c in [q_copy, own_done] + last:
        c.wait()


def prefix_parts(hidden, cs, w_q, w_uk, kv_prefix, scale2, chips):
    rows, depth = hidden.shape
    heads, nope, lat = w_uk.shape
    rope = w_q.shape[1] // heads - nope
    steps, sub = 4, 512
    wide = w_q.shape[1] // steps
    flat = heads * rows
    keys = CORES * kv_prefix.shape[1]
    others = chips - 1
    full, half = (flat + 8, lat), (flat // 2 + 8, lat)
    dma = pltpu.SemaphoreType.DMA
    return pl.pallas_call(
        functools.partial(prefix_kernel, chips, scale2),
        out_shape=[jax.ShapeDtypeStruct((flat, lat + rope), BF16)] + [jax.ShapeDtypeStruct(full, F32)] * 3,
        in_specs=[VMEM, VMEM, HBM, HBM, HBM],
        out_specs=[HBM] * 4,
        scratch_shapes=[
            pltpu.VMEM((others, rows, depth), BF16), pltpu.VMEM((others, rows, 2 * rope), F32),
            pltpu.VMEM((steps, depth, wide), BF16), pltpu.VMEM(w_uk.shape, BF16),
            pltpu.VMEM((kv_prefix.shape[0], keys), BF16), pltpu.VMEM((chips, flat, lat + rope), BF16),
            pltpu.VMEM((3,) + full, F32), pltpu.VMEM((2,) + half, F32), pltpu.VMEM((2,) + half, F32),
            pltpu.VMEM((2, flat, sub), F32), pltpu.VMEM((2, flat, sub), BF16), pltpu.VMEM((flat, lat), F32)]
            + [pltpu.VMEM((flat, 128), F32)] * 3
            + [dma((steps,)), dma, dma, dma((4,)), dma((others,)), dma((others,)), dma((others,)), dma((others,)), dma, dma, dma((2,)), dma((2,))],
        compiler_params=pltpu.CompilerParams(collective_id=0, has_side_effects=True, vmem_limit_bytes=60 * 2**20),
        cost_estimate=pl.CostEstimate(flops=2 * chips * flat * keys * (768 + lat), bytes_accessed=2 * w_q.size, transcendentals=chips * flat * keys),
        name='prefix',
    )(hidden, cs, w_q, w_uk, kv_prefix)


def suffix_kernel(scale2, lat, heads, unroll, lens_ref, q_ref, kv_hbm, o_ref, m_out, l_out, q_buf, acc_ref, bufs, sems):
    seqs = q_ref.shape[0] // heads
    width = q_ref.shape[1]
    depth, size = bufs.shape[0], bufs.shape[2]
    lanes = [(k, min(k + 128, width)) for k in range(0, width, 128)]

    total = lax.fori_loop(0, seqs, lambda b, n: n + lens_ref[b] // size + 1, 0)

    def advance(b, j):
        last = j >= lens_ref[jnp.minimum(b, seqs - 1)] // size
        return jnp.where(last, b + 1, b), jnp.where(last, 0, j + 1)

    def rows_of(b):
        return pl.ds(jnp.minimum(b, seqs - 1), heads, stride=seqs)

    def copy(b, j, slot):
        return pltpu.make_async_copy(kv_hbm.at[b, :, pl.ds(pl.multiple_of(j * size, size), size)], bufs.at[slot], sems.at[slot])

    def scores(b, slot):
        q = jnp.concatenate([q_buf[n, rows_of(b), :][:, 0:hi - lo] for n, (lo, hi) in enumerate(lanes)], axis=1).astype(BF16)
        return jnp.dot(q, bufs[slot], preferred_element_type=F32)

    zero = jnp.int32(0)
    items = [(zero, zero)]
    for n in range(depth - unroll):
        copy(*items[n], n).start()
        items.append(advance(*items[n]))
    for n, (lo, hi) in enumerate(lanes):
        q_buf[n, :, 0:hi - lo] = q_ref[:, lo:hi].astype(F32)
    acc_ref[...] = jnp.zeros_like(acc_ref)
    for n in range(unroll):
        copy(*items[n], n).wait()
    pos = lax.broadcasted_iota(jnp.int32, (heads, size), 1)

    def flush(b, n):
        for k in range(lat // 128):
            o_ref[k, rows_of(b), :] = acc_ref[n, :, k * 128:(k + 1) * 128]

    def absorb(b, j, slot, s, m, l, before, n):
        live = b < seqs
        limit = jnp.where(live, lens_ref[jnp.minimum(b, seqs - 1)] - j * size, -1)
        s2 = jnp.where(pos <= limit, s * scale2, -jnp.inf)
        m_old = jnp.where(jnp.logical_and(live, j == 0), -jnp.inf, m)
        m_new = jnp.maximum(m_old, jnp.max(s2, axis=1, keepdims=True))
        alpha = jnp.exp2(m_old - m_new)
        p = [jnp.exp2(s2[:, k:k + 128] - m_new) for k in range(0, size, 128)]
        l_new = l * alpha + functools.reduce(jnp.add, p)
        p = jnp.concatenate([x.astype(BF16) for x in p], axis=1)
        pv = lax.dot_general(p, bufs[slot, 0:lat, :], NT, preferred_element_type=F32)
        for k in range(0, lat, 128):
            acc_ref[n, :, k:k + 128] = acc_ref[before, :, k:k + 128] * alpha + pv[:, k:k + 128]
        m_out[rows_of(b), :] = m_new
        l_out[rows_of(b), :] = l_new
        return m_new, l_new

    def body(i, carry):
        prev, now, later, fetching, s_now, m, l = carry
        t = unroll * i
        for n in range(unroll):
            @pl.when(t + depth - unroll + n < total)
            def _():
                copy(*fetching, lax.rem(t + depth - unroll + n, depth)).start()
            fetching = advance(*fetching)
        for n in range(unroll):
            @pl.when(t + unroll + n < total)
            def _():
                copy(*later[n], lax.rem(t + unroll + n, depth)).wait()
        for n in range(unroll):
            flush(prev[n], n)
        s_next = [scores(later[n][0], lax.rem(t + unroll + n, depth)) for n in range(unroll)]
        for n in range(unroll):
            m, l = absorb(*now[n], lax.rem(t + n, depth), s_now[n], m, l, (n - 1) % unroll, n)
        coming = [advance(*later[-1])]
        for n in range(1, unroll):
            coming.append(advance(*coming[-1]))
        return [b for b, _ in now], later, coming, fetching, s_next, m, l

    later = items[unroll:2 * unroll]
    s_now = [scores(items[n][0], n) for n in range(unroll)]
    stat = jnp.zeros((heads, 128), F32)
    first = [items[0][0]] * unroll
    carry = (first, items[:unroll], later, items[-1], s_now, stat, stat)
    carry = lax.fori_loop(0, (total + unroll - 1) // unroll, body, carry)
    for n in range(unroll):
        flush(carry[0][n], n)


def suffix_part(q_rows, kv_suffix, seq_lens, heads, scale2, lat):
    rows, width = q_rows.shape
    seqs, _, slots = kv_suffix.shape
    size, depth, unroll = 512, 16, 4
    stat = jax.ShapeDtypeStruct((rows, 128), F32)
    return pl.pallas_call(
        functools.partial(suffix_kernel, scale2, lat, heads, unroll),
        out_shape=[jax.ShapeDtypeStruct((lat // 128, rows, 128), F32), stat, stat],
        in_specs=[SMEM, VMEM, HBM],
        out_specs=[VMEM, VMEM, VMEM],
        scratch_shapes=[pltpu.VMEM((-(-width // 128), rows, 128), F32), pltpu.VMEM((unroll, heads, lat), F32), pltpu.VMEM((depth, width, size), BF16), pltpu.SemaphoreType.DMA((depth,))],
        compiler_params=pltpu.CompilerParams(vmem_limit_bytes=32 * 2**20),
        cost_estimate=pl.CostEstimate(flops=2 * seqs * slots * 256 * 768, bytes_accessed=seqs * slots * width * 2, transcendentals=seqs * slots * heads),
        name='suffix',
    )(seq_lens, q_rows, kv_suffix)


def stats_of(ref, size):
    both = ref[size:size + 8, 0:size].T
    return both[:, 0:1], both[:, 1:2]


def output_kernel(hid_ref, os_ref, ms_ref, ls_ref, *refs):
    parts, (uv_ref, wo_ref, out_ref, v_buf) = refs[:3], refs[3:]
    rows, heads = hid_ref.shape[0], uv_ref.shape[0]
    lat, width = uv_ref.shape[1], uv_ref.shape[2]
    flat = rows * heads
    stats = [stats_of(ref, flat) for ref in parts]
    for h in range(heads):
        cut = slice(h * rows, (h + 1) * rows)
        m_s, l_s = ms_ref[cut, 0:1], jnp.sum(ls_ref[cut, :], axis=1, keepdims=True)
        ms = [m_s] + [m[cut] for m, _ in stats]
        ls = [l_s] + [l[cut] for _, l in stats]
        m_all = functools.reduce(jnp.maximum, ms)
        ws = [jnp.exp2(m - m_all) for m in ms]
        l_all = functools.reduce(jnp.add, [l * w for l, w in zip(ls, ws)])
        o_s = jnp.concatenate([os_ref[n, cut, :] for n in range(lat // 128)], axis=1)
        o_all = o_s * ws[0]
        for ref, w in zip(parts, ws[1:]):
            o_all = o_all + ref[cut, :] * w
        o_h = (o_all / l_all).astype(BF16)
        v_buf[:, h * width:(h + 1) * width] = jnp.dot(o_h, uv_ref[h], preferred_element_type=F32).astype(BF16)
    proj = jnp.dot(v_buf[...], wo_ref[...], preferred_element_type=F32)
    out_ref[...] = (hid_ref[...].astype(F32) + proj).astype(BF16)


def output_part(hidden, suffix, parts, w_uv, w_o):
    rows = hidden.shape[0]
    heads, lat, val = w_uv.shape
    return pl.pallas_call(
        output_kernel,
        out_shape=jax.ShapeDtypeStruct(hidden.shape, BF16),
        in_specs=[VMEM] * 9,
        out_specs=VMEM,
        scratch_shapes=[pltpu.VMEM((rows, heads * val), BF16)],
        compiler_params=pltpu.CompilerParams(vmem_limit_bytes=24 * 2**20),
        cost_estimate=pl.CostEstimate(flops=2 * rows * heads * val * (lat + hidden.shape[1]), bytes_accessed=2 * (w_uv.size + w_o.size), transcendentals=0),
        name='output',
    )(hidden, *suffix, *parts, w_uv, w_o)


def solution(mesh):
    group = mesh.shape['ctx']
    chips = group // CORES
    rows_spec = P(('dp', 'ctx'), None)
    whole_spec = P()

    def local_step(hidden, w_q, w_uk, w_uv, w_o, kv_prefix, kv_suffix, seq_lens):
        rows = hidden.shape[0]
        heads, nope, lat = w_uk.shape
        head_w = w_q.shape[1] // heads
        rope = head_w - nope
        prefix_len = kv_prefix.shape[0] * group
        scale2 = head_w ** -0.5 * LOG2E
        kv_prefix = kv_prefix.T
        kv_suffix = kv_suffix.transpose(0, 2, 1)
        cs = rope_table(prefix_len + seq_lens, rope // 2)
        query, own, up, down = prefix_parts(hidden, cs, w_q, w_uk, kv_prefix, scale2, chips)

        def send(value, hop):
            return lax.ppermute(value, 'ctx', [(j, (j + hop * CORES) % group) for j in range(group)])

        in_up, in_down = send(up, 1), send(down, -1)
        suffix = suffix_part(query, kv_suffix, seq_lens, heads, scale2, lat)
        return output_part(hidden, suffix, (own, in_up, in_down), w_uv, w_o)

    return jax.shard_map(local_step, mesh=mesh, in_specs=(rows_spec, whole_spec, whole_spec, whole_spec, whole_spec, rows_spec, P(('dp', 'ctx'), None, None), P(('dp', 'ctx'))), out_specs=rows_spec, check_vma=False)
```

```python
import functools
import math
import jax
import jax.numpy as jnp
from jax import lax
from jax.experimental import pallas as pl
from jax.experimental.pallas import tpu as pltpu
from jax.sharding import PartitionSpec as P

ROPE_BASE = 10000
LOG2E = math.log2(math.e)
CORES = 2
F32 = jnp.float32
BF16 = jnp.bfloat16
HBM = pl.BlockSpec(memory_space=pltpu.HBM)
VMEM = pl.BlockSpec(memory_space=pltpu.VMEM)
SMEM = pl.BlockSpec(memory_space=pltpu.SMEM)
NT = (((1,), (1,)), ((), ()))


def rope_table(positions, half_dim):
    lane = jnp.arange(4 * half_dim)
    inv_freq = jnp.exp((lane % half_dim).astype(F32) * (-math.log(ROPE_BASE) / half_dim))
    angle = positions.astype(F32)[:, None] * inv_freq
    return jnp.where(lane < 2 * half_dim, jnp.cos(angle), jnp.sin(angle))


def prefix_part(scale2, lat, q_ref, k_ref, outs, work, hook=None, loaded=False, next_ref=None):
    s_ref, p_ref, acc_ref, a_ref, m_ref, l_ref = work
    rows, sub = q_ref.shape[0], s_ref.shape[2]
    count = k_ref.shape[1] // sub
    chunk = 64
    m_ref[...] = jnp.full_like(m_ref, -jnp.inf)
    l_ref[...] = jnp.zeros_like(l_ref)
    acc_ref[...] = jnp.zeros_like(acc_ref)

    def keys(n):
        return pl.ds(pl.multiple_of(n * sub, sub), sub)

    def scores(n, slot, ref=q_ref):
        s_ref[slot] = jnp.dot(ref[...], k_ref[:, keys(n)], preferred_element_type=F32)

    def absorb(n, slot):
        for r in range(0, rows, chunk):
            cut = slice(r, r + chunk)
            s = s_ref[slot, cut, :]
            m_old = m_ref[cut, :]
            m_new = jnp.maximum(m_old, jnp.max(s, axis=1, keepdims=True) * scale2)
            alpha = jnp.exp2(m_old - m_new)
            l_new = l_ref[cut, :] * alpha
            for k in range(0, sub, 128):
                p = jnp.exp2(s[:, k:k + 128] * scale2 - m_new)
                l_new = l_new + p
                p_ref[slot, cut, k:k + 128] = p.astype(BF16)
            l_ref[cut, :] = l_new
            m_ref[cut, :] = m_new
            a_ref[cut, :] = alpha
        pv = lax.dot_general(p_ref[slot], k_ref[0:lat, keys(n)], NT, preferred_element_type=F32)
        alpha = a_ref[...]
        for k in range(0, lat, 128):
            acc_ref[:, k:k + 128] = acc_ref[:, k:k + 128] * alpha + pv[:, k:k + 128]

    if not loaded:
        scores(0, 0)
    if hook is not None:
        hook()

    def pair(i, carry):
        scores(2 * i + 1, 1)
        absorb(2 * i, 0)
        scores(2 * i + 2, 0)
        absorb(2 * i + 1, 1)
        return carry

    lax.fori_loop(0, count // 2 - 1, pair, 0)
    scores(count - 1, 1)
    absorb(count - 2, 0)
    if next_ref is not None:
        scores(0, 0, next_ref)
    absorb(count - 1, 1)
    m_t = m_ref[...].T[0:1]
    l_t = jnp.broadcast_to(jnp.sum(l_ref[...], axis=1, keepdims=True), (rows, 128)).T[0:1]
    size = rows // len(outs)
    for k, ref in enumerate(outs):
        cut = slice(k * size, (k + 1) * size)
        ref[0:size, :] = acc_ref[cut, :]
        ref[size:size + 1, 0:size] = m_t[:, cut]
        ref[size + 1:size + 2, 0:size] = l_t[:, cut]


def merge_into(x_ref, y_ref, offset):
    rows, half = x_ref.shape[0] - 8, y_ref.shape[0] - 8
    cut = slice(offset, offset + half)
    m_x, m_y = x_ref[rows:rows + 1, cut], y_ref[half:half + 1, 0:half]
    l_x, l_y = x_ref[rows + 1:rows + 2, cut], y_ref[half + 1:half + 2, 0:half]
    m_all = jnp.maximum(m_x, m_y)
    w_x, w_y = jnp.exp2(m_x - m_all), jnp.exp2(m_y - m_all)
    x_ref[rows:rows + 1, cut] = m_all
    x_ref[rows + 1:rows + 2, cut] = l_x * w_x + l_y * w_y
    c_x = jnp.broadcast_to(w_x, (8, half)).T[:, 0:1]
    c_y = jnp.broadcast_to(w_y, (8, half)).T[:, 0:1]
    x_ref[cut, :] = x_ref[cut, :] * c_x + y_ref[0:half, :] * c_y


def prefix_kernel(chips, scale2, hid_ref, cs_ref, wq_hbm, wuk_hbm, kv_hbm, q_out, own_out, up_out, down_out,
                  hid_all, cs_all, wq_buf, wuk_buf, k_ref, q_buf, res, far, got,
                  s_ref, p_ref, acc_ref, a_ref, m_ref, l_ref,
                  wq_sem, wuk_sem, kv_sem, out_sem, hid_send, hid_recv, cs_send, cs_recv, kv_send, kv_recv, far_send, far_recv):
    me = lax.axis_index('ctx')
    chip, core = me // CORES, me % CORES
    steps, _, wide = wq_buf.shape
    rows = hid_ref.shape[0]
    heads, nope, lat = wuk_buf.shape
    rope = q_buf.shape[2] - lat
    head_w = nope + rope
    keys = kv_hbm.shape[1]
    per = wide // head_w
    work = (s_ref, p_ref, acc_ref, a_ref, m_ref, l_ref)

    def weight_copy(i):
        return pltpu.make_async_copy(wq_hbm.at[:, pl.ds(i * wide, wide)], wq_buf.at[i], wq_sem.at[i])

    def remote(src, dst, send, recv, dev):
        return pltpu.make_async_remote_copy(src, dst, send, recv, device_id={'ctx': dev}, device_id_type=pl.DeviceIdType.MESH)

    weight_copy(0).start()
    uk_copy = pltpu.make_async_copy(wuk_hbm, wuk_buf, wuk_sem)
    uk_copy.start()
    for i in range(1, steps):
        weight_copy(i).start()
    own_copy = pltpu.make_async_copy(kv_hbm, k_ref.at[:, pl.ds(0, keys)], kv_sem)
    own_copy.start()
    partner = chip * CORES + (1 - core)
    peers = [((chip + chips - r) % chips) * CORES + core for r in range(1, chips)]
    barrier = pltpu.get_barrier_semaphore()
    for dev in [partner] + peers:
        pl.semaphore_signal(barrier, inc=1, device_id={'ctx': dev}, device_id_type=pl.DeviceIdType.MESH)
    pl.semaphore_wait(barrier, chips)
    copies = []
    for r in range(1, chips):
        copies.append(remote(hid_ref, hid_all.at[r - 1], hid_send.at[r - 1], hid_recv.at[r - 1], peers[r - 1]))
        copies.append(remote(cs_ref, cs_all.at[r - 1], cs_send.at[r - 1], cs_recv.at[r - 1], peers[r - 1]))
    kv_copy = remote(kv_hbm, k_ref.at[:, pl.ds(keys, keys)], kv_send, kv_recv, partner)
    kv_copy.start()
    for c in copies:
        c.start()

    def queries(x, cs, first, own):
        cos, sin = cs[:, :rope], cs[:, rope:]
        for i in range(steps):
            if own:
                weight_copy(i).wait()
            qa = jnp.dot(x, wq_buf[i], preferred_element_type=F32).astype(BF16)
            if own and i == 0:
                uk_copy.wait()
            for k in range(per):
                h = i * per + k
                q_lat = jnp.dot(qa[:, k * head_w:k * head_w + nope], wuk_buf[h], preferred_element_type=F32).astype(BF16)
                pe = qa[:, k * head_w + nope:(k + 1) * head_w].astype(F32)
                turned = jnp.concatenate([-pe[:, rope // 2:], pe[:, :rope // 2]], axis=1)
                pe = (pe * cos + turned * sin).astype(BF16)
                for r in range(x.shape[0] // rows):
                    q_buf[first + r, h * rows:(h + 1) * rows, 0:lat] = q_lat[r * rows:(r + 1) * rows]
                    q_buf[first + r, h * rows:(h + 1) * rows, lat:lat + rope] = pe[r * rows:(r + 1) * rows]

    queries(hid_ref[...], cs_ref[...], 0, True)
    q_copy = pltpu.make_async_copy(q_buf.at[0], q_out, out_sem.at[0])
    own_copy.wait()
    kv_copy.wait()
    prefix_part(scale2, lat, q_buf.at[0], k_ref, [res.at[0]], work, q_copy.start)
    for c in copies:
        c.wait()
    queries(hid_all[...].reshape((chips - 1) * rows, hid_ref.shape[1]), cs_all[...].reshape((chips - 1) * rows, 2 * rope), 1, False)
    own_done = pltpu.make_async_copy(res.at[0], own_out, out_sem.at[1])
    prefix_part(scale2, lat, q_buf.at[2], k_ref, [far.at[0], far.at[1]], work, own_done.start, next_ref=q_buf.at[1])
    sends = [remote(far.at[n], got.at[n], far_send.at[n], far_recv.at[n], dev) for n, dev in enumerate((peers[2], peers[0]))]

    def send_far():
        for c in sends:
            c.start()

    prefix_part(scale2, lat, q_buf.at[1], k_ref, [res.at[1]], work, send_far, loaded=True, next_ref=q_buf.at[3])
    prefix_part(scale2, lat, q_buf.at[3], k_ref, [res.at[2]], work, loaded=True)
    for c in sends:
        c.wait()
    merge_into(res.at[1], got.at[0], 0)
    merge_into(res.at[2], got.at[1], heads * rows // 2)
    last = [pltpu.make_async_copy(res.at[1], up_out, out_sem.at[2]), pltpu.make_async_copy(res.at[2], down_out, out_sem.at[3])]
    for c in last:
        c.start()
    for c in [q_copy, own_done] + last:
        c.wait()


def prefix_parts(hidden, cs, w_q, w_uk, kv_prefix, scale2, chips):
    rows, depth = hidden.shape
    heads, nope, lat = w_uk.shape
    rope = w_q.shape[1] // heads - nope
    steps, sub = 4, 1024
    wide = w_q.shape[1] // steps
    flat = heads * rows
    keys = CORES * kv_prefix.shape[1]
    others = chips - 1
    full, half = (flat + 8, lat), (flat // 2 + 8, lat)
    dma = pltpu.SemaphoreType.DMA
    return pl.pallas_call(
        functools.partial(prefix_kernel, chips, scale2),
        out_shape=[jax.ShapeDtypeStruct((flat, lat + rope), BF16)] + [jax.ShapeDtypeStruct(full, F32)] * 3,
        in_specs=[VMEM, VMEM, HBM, HBM, HBM],
        out_specs=[HBM] * 4,
        scratch_shapes=[
            pltpu.VMEM((others, rows, depth), BF16), pltpu.VMEM((others, rows, 2 * rope), F32),
            pltpu.VMEM((steps, depth, wide), BF16), pltpu.VMEM(w_uk.shape, BF16),
            pltpu.VMEM((kv_prefix.shape[0], keys), BF16), pltpu.VMEM((chips, flat, lat + rope), BF16),
            pltpu.VMEM((3,) + full, F32), pltpu.VMEM((2,) + half, F32), pltpu.VMEM((2,) + half, F32),
            pltpu.VMEM((2, flat, sub), F32), pltpu.VMEM((2, flat, sub), BF16), pltpu.VMEM((flat, lat), F32)]
            + [pltpu.VMEM((flat, 128), F32)] * 3
            + [dma((steps,)), dma, dma, dma((4,)), dma((others,)), dma((others,)), dma((others,)), dma((others,)), dma, dma, dma((2,)), dma((2,))],
        compiler_params=pltpu.CompilerParams(collective_id=0, has_side_effects=True, vmem_limit_bytes=60 * 2**20),
        cost_estimate=pl.CostEstimate(flops=2 * chips * flat * keys * (768 + lat), bytes_accessed=2 * w_q.size, transcendentals=chips * flat * keys),
        name='prefix',
    )(hidden, cs, w_q, w_uk, kv_prefix)


def suffix_kernel(scale2, lat, heads, unroll, lens_ref, q_ref, kv_hbm, o_ref, m_out, l_out, q_buf, acc_ref, bufs, sems):
    seqs = q_ref.shape[0] // heads
    width = q_ref.shape[1]
    depth, size = bufs.shape[0], bufs.shape[2]
    lanes = [(k, min(k + 128, width)) for k in range(0, width, 128)]

    total = lax.fori_loop(0, seqs, lambda b, n: n + lens_ref[b] // size + 1, 0)

    def advance(b, j):
        last = j >= lens_ref[jnp.minimum(b, seqs - 1)] // size
        return jnp.where(last, b + 1, b), jnp.where(last, 0, j + 1)

    def rows_of(b):
        return pl.ds(jnp.minimum(b, seqs - 1), heads, stride=seqs)

    def copy(b, j, slot):
        return pltpu.make_async_copy(kv_hbm.at[b, :, pl.ds(pl.multiple_of(j * size, size), size)], bufs.at[slot], sems.at[slot])

    def scores(b, slot):
        q = jnp.concatenate([q_buf[n, rows_of(b), :][:, 0:hi - lo] for n, (lo, hi) in enumerate(lanes)], axis=1).astype(BF16)
        return jnp.dot(q, bufs[slot], preferred_element_type=F32)

    zero = jnp.int32(0)
    items = [(zero, zero)]
    for n in range(depth - unroll):
        copy(*items[n], n).start()
        items.append(advance(*items[n]))
    for n, (lo, hi) in enumerate(lanes):
        q_buf[n, :, 0:hi - lo] = q_ref[:, lo:hi].astype(F32)
    acc_ref[...] = jnp.zeros_like(acc_ref)
    for n in range(unroll):
        copy(*items[n], n).wait()
    pos = lax.broadcasted_iota(jnp.int32, (heads, size), 1)

    def flush(b, n):
        for k in range(lat // 128):
            o_ref[k, rows_of(b), :] = acc_ref[n, :, k * 128:(k + 1) * 128]

    def absorb(b, j, slot, s, m, l, before, n):
        live = b < seqs
        limit = jnp.where(live, lens_ref[jnp.minimum(b, seqs - 1)] - j * size, -1)
        s2 = jnp.where(pos <= limit, s * scale2, -jnp.inf)
        m_old = jnp.where(jnp.logical_and(live, j == 0), -jnp.inf, m)
        m_new = jnp.maximum(m_old, jnp.max(s2, axis=1, keepdims=True))
        alpha = jnp.exp2(m_old - m_new)
        p = [jnp.exp2(s2[:, k:k + 128] - m_new) for k in range(0, size, 128)]
        l_new = l * alpha + functools.reduce(jnp.add, p)
        p = jnp.concatenate([x.astype(BF16) for x in p], axis=1)
        pv = lax.dot_general(p, bufs[slot, 0:lat, :], NT, preferred_element_type=F32)
        for k in range(0, lat, 128):
            acc_ref[n, :, k:k + 128] = acc_ref[before, :, k:k + 128] * alpha + pv[:, k:k + 128]
        m_out[rows_of(b), :] = m_new
        l_out[rows_of(b), :] = l_new
        return m_new, l_new

    def body(i, carry):
        prev, now, later, fetching, s_now, m, l = carry
        t = unroll * i
        for n in range(unroll):
            @pl.when(t + depth - unroll + n < total)
            def _():
                copy(*fetching, lax.rem(t + depth - unroll + n, depth)).start()
            fetching = advance(*fetching)
        for n in range(unroll):
            @pl.when(t + unroll + n < total)
            def _():
                copy(*later[n], lax.rem(t + unroll + n, depth)).wait()
        for n in range(unroll):
            flush(prev[n], n)
        s_next = [scores(later[n][0], lax.rem(t + unroll + n, depth)) for n in range(unroll)]
        for n in range(unroll):
            m, l = absorb(*now[n], lax.rem(t + n, depth), s_now[n], m, l, (n - 1) % unroll, n)
        coming = [advance(*later[-1])]
        for n in range(1, unroll):
            coming.append(advance(*coming[-1]))
        return [b for b, _ in now], later, coming, fetching, s_next, m, l

    later = items[unroll:2 * unroll]
    s_now = [scores(items[n][0], n) for n in range(unroll)]
    stat = jnp.zeros((heads, 128), F32)
    first = [items[0][0]] * unroll
    carry = (first, items[:unroll], later, items[-1], s_now, stat, stat)
    carry = lax.fori_loop(0, (total + unroll - 1) // unroll, body, carry)
    for n in range(unroll):
        flush(carry[0][n], n)


def suffix_part(q_rows, kv_suffix, seq_lens, heads, scale2, lat):
    rows, width = q_rows.shape
    seqs, _, slots = kv_suffix.shape
    size, depth, unroll = 512, 16, 4
    stat = jax.ShapeDtypeStruct((rows, 128), F32)
    return pl.pallas_call(
        functools.partial(suffix_kernel, scale2, lat, heads, unroll),
        out_shape=[jax.ShapeDtypeStruct((lat // 128, rows, 128), F32), stat, stat],
        in_specs=[SMEM, VMEM, HBM],
        out_specs=[VMEM, VMEM, VMEM],
        scratch_shapes=[pltpu.VMEM((-(-width // 128), rows, 128), F32), pltpu.VMEM((unroll, heads, lat), F32), pltpu.VMEM((depth, width, size), BF16), pltpu.SemaphoreType.DMA((depth,))],
        compiler_params=pltpu.CompilerParams(vmem_limit_bytes=32 * 2**20),
        cost_estimate=pl.CostEstimate(flops=2 * seqs * slots * 256 * 768, bytes_accessed=seqs * slots * width * 2, transcendentals=seqs * slots * heads),
        name='suffix',
    )(seq_lens, q_rows, kv_suffix)


def stats_of(ref, size):
    both = ref[size:size + 8, 0:size].T
    return both[:, 0:1], both[:, 1:2]


def output_kernel(hid_ref, os_ref, ms_ref, ls_ref, *refs):
    parts, (uv_ref, wo_ref, out_ref, v_buf) = refs[:3], refs[3:]
    rows, heads = hid_ref.shape[0], uv_ref.shape[0]
    lat, width = uv_ref.shape[1], uv_ref.shape[2]
    flat = rows * heads
    stats = [stats_of(ref, flat) for ref in parts]
    for h in range(heads):
        cut = slice(h * rows, (h + 1) * rows)
        m_s, l_s = ms_ref[cut, 0:1], jnp.sum(ls_ref[cut, :], axis=1, keepdims=True)
        ms = [m_s] + [m[cut] for m, _ in stats]
        ls = [l_s] + [l[cut] for _, l in stats]
        m_all = functools.reduce(jnp.maximum, ms)
        ws = [jnp.exp2(m - m_all) for m in ms]
        l_all = functools.reduce(jnp.add, [l * w for l, w in zip(ls, ws)])
        o_s = jnp.concatenate([os_ref[n, cut, :] for n in range(lat // 128)], axis=1)
        o_all = o_s * ws[0]
        for ref, w in zip(parts, ws[1:]):
            o_all = o_all + ref[cut, :] * w
        o_h = (o_all / l_all).astype(BF16)
        v_buf[:, h * width:(h + 1) * width] = jnp.dot(o_h, uv_ref[h], preferred_element_type=F32).astype(BF16)
    proj = jnp.dot(v_buf[...], wo_ref[...], preferred_element_type=F32)
    out_ref[...] = (hid_ref[...].astype(F32) + proj).astype(BF16)


def output_part(hidden, suffix, parts, w_uv, w_o):
    rows = hidden.shape[0]
    heads, lat, val = w_uv.shape
    return pl.pallas_call(
        output_kernel,
        out_shape=jax.ShapeDtypeStruct(hidden.shape, BF16),
        in_specs=[VMEM] * 9,
        out_specs=VMEM,
        scratch_shapes=[pltpu.VMEM((rows, heads * val), BF16)],
        compiler_params=pltpu.CompilerParams(vmem_limit_bytes=24 * 2**20),
        cost_estimate=pl.CostEstimate(flops=2 * rows * heads * val * (lat + hidden.shape[1]), bytes_accessed=2 * (w_uv.size + w_o.size), transcendentals=0),
        name='output',
    )(hidden, *suffix, *parts, w_uv, w_o)


def solution(mesh):
    group = mesh.shape['ctx']
    chips = group // CORES
    rows_spec = P(('dp', 'ctx'), None)
    whole_spec = P()

    def local_step(hidden, w_q, w_uk, w_uv, w_o, kv_prefix, kv_suffix, seq_lens):
        rows = hidden.shape[0]
        heads, nope, lat = w_uk.shape
        head_w = w_q.shape[1] // heads
        rope = head_w - nope
        prefix_len = kv_prefix.shape[0] * group
        scale2 = head_w ** -0.5 * LOG2E
        kv_prefix = kv_prefix.T
        kv_suffix = kv_suffix.transpose(0, 2, 1)
        cs = rope_table(prefix_len + seq_lens, rope // 2)
        query, own, up, down = prefix_parts(hidden, cs, w_q, w_uk, kv_prefix, scale2, chips)

        def send(value, hop):
            return lax.ppermute(value, 'ctx', [(j, (j + hop * CORES) % group) for j in range(group)])

        in_up, in_down = send(up, 1), send(down, -1)
        suffix = suffix_part(query, kv_suffix, seq_lens, heads, scale2, lat)
        return output_part(hidden, suffix, (own, in_up, in_down), w_uv, w_o)

    return jax.shard_map(local_step, mesh=mesh, in_specs=(rows_spec, whole_spec, whole_spec, whole_spec, whole_spec, rows_spec, P(('dp', 'ctx'), None, None), P(('dp', 'ctx'))), out_specs=rows_spec, check_vma=False)
```

```python
import functools
import math
import jax
import jax.numpy as jnp
from jax import lax
from jax.experimental import pallas as pl
from jax.experimental.pallas import tpu as pltpu
from jax.sharding import PartitionSpec as P

ROPE_BASE = 10000
LOG2E = math.log2(math.e)
CORES = 2
F32 = jnp.float32
BF16 = jnp.bfloat16
HBM = pl.BlockSpec(memory_space=pltpu.HBM)
VMEM = pl.BlockSpec(memory_space=pltpu.VMEM)
SMEM = pl.BlockSpec(memory_space=pltpu.SMEM)
NT = (((1,), (1,)), ((), ()))


TURN = (6.28125, 4059 / 2 ** 21, 2 * math.pi - 6.28125 - 4059 / 2 ** 21)


def rope_rates(half_dim):
    lane = jnp.arange(4 * half_dim) % half_dim
    return jnp.exp(lane.astype(F32) * (-math.log(ROPE_BASE) / half_dim))[None, :]


def rope_table(start, lens_ref, rate_ref, cs_ref):
    rows, width = cs_ref.shape
    for b in range(rows):
        cs_ref[b:b + 1, :] = jnp.full((1, width), start + lens_ref[b], jnp.int32).astype(F32)
    angle = cs_ref[...] * rate_ref[...]
    turns = jnp.floor(angle * (0.5 / math.pi) + 0.5)
    for part in TURN:
        angle = angle - turns * part
    lane = lax.broadcasted_iota(jnp.int32, (rows, width), 1)
    cs_ref[...] = jnp.where(lane < width // 2, jnp.cos(angle), jnp.sin(angle))


def prefix_part(scale2, lat, q_ref, k_ref, outs, work, hook=None, loaded=False, next_ref=None):
    s_ref, p_ref, acc_ref, a_ref, m_ref, l_ref = work
    rows, sub = q_ref.shape[0], s_ref.shape[2]
    count = k_ref.shape[1] // sub
    chunk = 64
    m_ref[...] = jnp.full_like(m_ref, -jnp.inf)
    l_ref[...] = jnp.zeros_like(l_ref)
    acc_ref[...] = jnp.zeros_like(acc_ref)

    def keys(n):
        return pl.ds(pl.multiple_of(n * sub, sub), sub)

    def scores(n, slot, ref=q_ref):
        s_ref[slot] = jnp.dot(ref[...], k_ref[:, keys(n)], preferred_element_type=F32)

    def absorb(n, slot):
        for r in range(0, rows, chunk):
            cut = slice(r, r + chunk)
            s = s_ref[slot, cut, :]
            m_old = m_ref[cut, :]
            m_new = jnp.maximum(m_old, jnp.max(s, axis=1, keepdims=True) * scale2)
            alpha = jnp.exp2(m_old - m_new)
            l_new = l_ref[cut, :] * alpha
            for k in range(0, sub, 128):
                p = jnp.exp2(s[:, k:k + 128] * scale2 - m_new)
                l_new = l_new + p
                p_ref[slot, cut, k:k + 128] = p.astype(BF16)
            l_ref[cut, :] = l_new
            m_ref[cut, :] = m_new
            a_ref[cut, :] = alpha
        pv = lax.dot_general(p_ref[slot], k_ref[0:lat, keys(n)], NT, preferred_element_type=F32)
        alpha = a_ref[...]
        for k in range(0, lat, 128):
            acc_ref[:, k:k + 128] = acc_ref[:, k:k + 128] * alpha + pv[:, k:k + 128]

    if not loaded:
        scores(0, 0)
    if hook is not None:
        hook()

    def pair(i, carry):
        scores(2 * i + 1, 1)
        absorb(2 * i, 0)
        scores(2 * i + 2, 0)
        absorb(2 * i + 1, 1)
        return carry

    lax.fori_loop(0, count // 2 - 1, pair, 0)
    scores(count - 1, 1)
    absorb(count - 2, 0)
    if next_ref is not None:
        scores(0, 0, next_ref)
    absorb(count - 1, 1)
    m_t = m_ref[...].T[0:1]
    l_t = jnp.broadcast_to(jnp.sum(l_ref[...], axis=1, keepdims=True), (rows, 128)).T[0:1]
    size = rows // len(outs)
    for k, ref in enumerate(outs):
        cut = slice(k * size, (k + 1) * size)
        ref[0:size, :] = acc_ref[cut, :]
        ref[size:size + 1, 0:size] = m_t[:, cut]
        ref[size + 1:size + 2, 0:size] = l_t[:, cut]


def merge_into(x_ref, y_ref, offset):
    rows, half = x_ref.shape[0] - 8, y_ref.shape[0] - 8
    cut = slice(offset, offset + half)
    m_x, m_y = x_ref[rows:rows + 1, cut], y_ref[half:half + 1, 0:half]
    l_x, l_y = x_ref[rows + 1:rows + 2, cut], y_ref[half + 1:half + 2, 0:half]
    m_all = jnp.maximum(m_x, m_y)
    w_x, w_y = jnp.exp2(m_x - m_all), jnp.exp2(m_y - m_all)
    x_ref[rows:rows + 1, cut] = m_all
    x_ref[rows + 1:rows + 2, cut] = l_x * w_x + l_y * w_y
    c_x = jnp.broadcast_to(w_x, (8, half)).T[:, 0:1]
    c_y = jnp.broadcast_to(w_y, (8, half)).T[:, 0:1]
    x_ref[cut, :] = x_ref[cut, :] * c_x + y_ref[0:half, :] * c_y


def prefix_kernel(chips, scale2, start, lens_ref, hid_ref, rate_ref, wq_hbm, wuk_hbm, kv_hbm, q_out, own_out, up_out, down_out,
                  hid_all, cs_ref, cs_all, wq_buf, wuk_buf, k_ref, q_buf, res, far, got,
                  s_ref, p_ref, acc_ref, a_ref, m_ref, l_ref,
                  wq_sem, wuk_sem, kv_sem, out_sem, hid_send, hid_recv, cs_send, cs_recv, kv_send, kv_recv, far_send, far_recv):
    me = lax.axis_index('ctx')
    chip, core = me // CORES, me % CORES
    steps, _, wide = wq_buf.shape
    rows = hid_ref.shape[0]
    heads, nope, lat = wuk_buf.shape
    rope = q_buf.shape[2] - lat
    head_w = nope + rope
    keys = kv_hbm.shape[1]
    per = wide // head_w
    work = (s_ref, p_ref, acc_ref, a_ref, m_ref, l_ref)

    def weight_copy(i):
        return pltpu.make_async_copy(wq_hbm.at[:, pl.ds(i * wide, wide)], wq_buf.at[i], wq_sem.at[i])

    def remote(src, dst, send, recv, dev):
        return pltpu.make_async_remote_copy(src, dst, send, recv, device_id={'ctx': dev}, device_id_type=pl.DeviceIdType.MESH)

    weight_copy(0).start()
    uk_copy = pltpu.make_async_copy(wuk_hbm, wuk_buf, wuk_sem)
    uk_copy.start()
    for i in range(1, steps):
        weight_copy(i).start()
    own_copy = pltpu.make_async_copy(kv_hbm, k_ref.at[:, pl.ds(0, keys)], kv_sem)
    own_copy.start()
    rope_table(start, lens_ref, rate_ref, cs_ref)
    partner = chip * CORES + (1 - core)
    peers = [((chip + chips - r) % chips) * CORES + core for r in range(1, chips)]
    barrier = pltpu.get_barrier_semaphore()
    for dev in [partner] + peers:
        pl.semaphore_signal(barrier, inc=1, device_id={'ctx': dev}, device_id_type=pl.DeviceIdType.MESH)
    pl.semaphore_wait(barrier, chips)
    copies = []
    for r in range(1, chips):
        copies.append(remote(hid_ref, hid_all.at[r - 1], hid_send.at[r - 1], hid_recv.at[r - 1], peers[r - 1]))
        copies.append(remote(cs_ref, cs_all.at[r - 1], cs_send.at[r - 1], cs_recv.at[r - 1], peers[r - 1]))
    kv_copy = remote(kv_hbm, k_ref.at[:, pl.ds(keys, keys)], kv_send, kv_recv, partner)
    kv_copy.start()
    for c in copies:
        c.start()

    def queries(x, cs, first, own):
        cos, sin = cs[:, :rope], cs[:, rope:]
        for i in range(steps):
            if own:
                weight_copy(i).wait()
            qa = jnp.dot(x, wq_buf[i], preferred_element_type=F32).astype(BF16)
            if own and i == 0:
                uk_copy.wait()
            for k in range(per):
                h = i * per + k
                q_lat = jnp.dot(qa[:, k * head_w:k * head_w + nope], wuk_buf[h], preferred_element_type=F32).astype(BF16)
                pe = qa[:, k * head_w + nope:(k + 1) * head_w].astype(F32)
                turned = jnp.concatenate([-pe[:, rope // 2:], pe[:, :rope // 2]], axis=1)
                pe = (pe * cos + turned * sin).astype(BF16)
                for r in range(x.shape[0] // rows):
                    q_buf[first + r, h * rows:(h + 1) * rows, 0:lat] = q_lat[r * rows:(r + 1) * rows]
                    q_buf[first + r, h * rows:(h + 1) * rows, lat:lat + rope] = pe[r * rows:(r + 1) * rows]

    queries(hid_ref[...], cs_ref[...], 0, True)
    q_copy = pltpu.make_async_copy(q_buf.at[0], q_out, out_sem.at[0])
    own_copy.wait()
    kv_copy.wait()
    prefix_part(scale2, lat, q_buf.at[0], k_ref, [res.at[0]], work, q_copy.start)
    for c in copies:
        c.wait()
    queries(hid_all[...].reshape((chips - 1) * rows, hid_ref.shape[1]), cs_all[...].reshape((chips - 1) * rows, 2 * rope), 1, False)
    own_done = pltpu.make_async_copy(res.at[0], own_out, out_sem.at[1])
    prefix_part(scale2, lat, q_buf.at[2], k_ref, [far.at[0], far.at[1]], work, own_done.start, next_ref=q_buf.at[1])
    sends = [remote(far.at[n], got.at[n], far_send.at[n], far_recv.at[n], dev) for n, dev in enumerate((peers[2], peers[0]))]

    def send_far():
        for c in sends:
            c.start()

    prefix_part(scale2, lat, q_buf.at[1], k_ref, [res.at[1]], work, send_far, loaded=True, next_ref=q_buf.at[3])
    prefix_part(scale2, lat, q_buf.at[3], k_ref, [res.at[2]], work, loaded=True)
    for c in sends:
        c.wait()
    merge_into(res.at[1], got.at[0], 0)
    merge_into(res.at[2], got.at[1], heads * rows // 2)
    last = [pltpu.make_async_copy(res.at[1], up_out, out_sem.at[2]), pltpu.make_async_copy(res.at[2], down_out, out_sem.at[3])]
    for c in last:
        c.start()
    for c in [q_copy, own_done] + last:
        c.wait()


def prefix_parts(hidden, seq_lens, w_q, w_uk, kv_prefix, scale2, chips):
    rows, depth = hidden.shape
    heads, nope, lat = w_uk.shape
    rope = w_q.shape[1] // heads - nope
    steps, sub = 4, 1024
    wide = w_q.shape[1] // steps
    flat = heads * rows
    keys = CORES * kv_prefix.shape[1]
    others = chips - 1
    full, half = (flat + 8, lat), (flat // 2 + 8, lat)
    dma = pltpu.SemaphoreType.DMA
    return pl.pallas_call(
        functools.partial(prefix_kernel, chips, scale2, chips * keys),
        out_shape=[jax.ShapeDtypeStruct((flat, lat + rope), BF16)] + [jax.ShapeDtypeStruct(full, F32)] * 3,
        in_specs=[SMEM, VMEM, VMEM, HBM, HBM, HBM],
        out_specs=[HBM] * 4,
        scratch_shapes=[
            pltpu.VMEM((others, rows, depth), BF16), pltpu.VMEM((rows, 2 * rope), F32), pltpu.VMEM((others, rows, 2 * rope), F32),
            pltpu.VMEM((steps, depth, wide), BF16), pltpu.VMEM(w_uk.shape, BF16),
            pltpu.VMEM((kv_prefix.shape[0], keys), BF16), pltpu.VMEM((chips, flat, lat + rope), BF16),
            pltpu.VMEM((3,) + full, F32), pltpu.VMEM((2,) + half, F32), pltpu.VMEM((2,) + half, F32),
            pltpu.VMEM((2, flat, sub), F32), pltpu.VMEM((2, flat, sub), BF16), pltpu.VMEM((flat, lat), F32)]
            + [pltpu.VMEM((flat, 128), F32)] * 3
            + [dma((steps,)), dma, dma, dma((4,)), dma((others,)), dma((others,)), dma((others,)), dma((others,)), dma, dma, dma((2,)), dma((2,))],
        compiler_params=pltpu.CompilerParams(collective_id=0, has_side_effects=True, vmem_limit_bytes=60 * 2**20),
        cost_estimate=pl.CostEstimate(flops=2 * chips * flat * keys * (768 + lat), bytes_accessed=2 * w_q.size, transcendentals=chips * flat * keys),
        name='prefix',
    )(seq_lens, hidden, rope_rates(rope // 2), w_q, w_uk, kv_prefix)


def suffix_kernel(scale2, lat, heads, unroll, lens_ref, q_ref, kv_hbm, o_ref, m_out, l_out, q_buf, acc_ref, bufs, sems):
    seqs = q_ref.shape[0] // heads
    width = q_ref.shape[1]
    depth, size = bufs.shape[0], bufs.shape[2]
    lanes = [(k, min(k + 128, width)) for k in range(0, width, 128)]

    total = lax.fori_loop(0, seqs, lambda b, n: n + lens_ref[b] // size + 1, 0)

    def advance(b, j):
        last = j >= lens_ref[jnp.minimum(b, seqs - 1)] // size
        return jnp.where(last, b + 1, b), jnp.where(last, 0, j + 1)

    def rows_of(b):
        return pl.ds(jnp.minimum(b, seqs - 1), heads, stride=seqs)

    def copy(b, j, slot):
        return pltpu.make_async_copy(kv_hbm.at[b, :, pl.ds(pl.multiple_of(j * size, size), size)], bufs.at[slot], sems.at[slot])

    def scores(b, slot):
        q = jnp.concatenate([q_buf[n, rows_of(b), :][:, 0:hi - lo] for n, (lo, hi) in enumerate(lanes)], axis=1).astype(BF16)
        return jnp.dot(q, bufs[slot], preferred_element_type=F32)

    zero = jnp.int32(0)
    items = [(zero, zero)]
    for n in range(depth - unroll):
        copy(*items[n], n).start()
        items.append(advance(*items[n]))
    for n, (lo, hi) in enumerate(lanes):
        q_buf[n, :, 0:hi - lo] = q_ref[:, lo:hi].astype(F32)
    acc_ref[...] = jnp.zeros_like(acc_ref)
    for n in range(unroll):
        copy(*items[n], n).wait()
    pos = lax.broadcasted_iota(jnp.int32, (heads, size), 1)

    def flush(b, n):
        for k in range(lat // 128):
            o_ref[k, rows_of(b), :] = acc_ref[n, :, k * 128:(k + 1) * 128]

    def absorb(b, j, slot, s, m, l, before, n):
        live = b < seqs
        limit = jnp.where(live, lens_ref[jnp.minimum(b, seqs - 1)] - j * size, -1)
        s2 = jnp.where(pos <= limit, s * scale2, -jnp.inf)
        m_old = jnp.where(jnp.logical_and(live, j == 0), -jnp.inf, m)
        m_new = jnp.maximum(m_old, jnp.max(s2, axis=1, keepdims=True))
        alpha = jnp.exp2(m_old - m_new)
        p = [jnp.exp2(s2[:, k:k + 128] - m_new) for k in range(0, size, 128)]
        l_new = l * alpha + functools.reduce(jnp.add, p)
        p = jnp.concatenate([x.astype(BF16) for x in p], axis=1)
        pv = lax.dot_general(p, bufs[slot, 0:lat, :], NT, preferred_element_type=F32)
        for k in range(0, lat, 128):
            acc_ref[n, :, k:k + 128] = acc_ref[before, :, k:k + 128] * alpha + pv[:, k:k + 128]
        m_out[rows_of(b), :] = m_new
        l_out[rows_of(b), :] = l_new
        return m_new, l_new

    def body(i, carry):
        prev, now, later, fetching, s_now, m, l = carry
        t = unroll * i
        for n in range(unroll):
            @pl.when(t + depth - unroll + n < total)
            def _():
                copy(*fetching, lax.rem(t + depth - unroll + n, depth)).start()
            fetching = advance(*fetching)
        for n in range(unroll):
            @pl.when(t + unroll + n < total)
            def _():
                copy(*later[n], lax.rem(t + unroll + n, depth)).wait()
        for n in range(unroll):
            flush(prev[n], n)
        s_next = [scores(later[n][0], lax.rem(t + unroll + n, depth)) for n in range(unroll)]
        for n in range(unroll):
            m, l = absorb(*now[n], lax.rem(t + n, depth), s_now[n], m, l, (n - 1) % unroll, n)
        coming = [advance(*later[-1])]
        for n in range(1, unroll):
            coming.append(advance(*coming[-1]))
        return [b for b, _ in now], later, coming, fetching, s_next, m, l

    later = items[unroll:2 * unroll]
    s_now = [scores(items[n][0], n) for n in range(unroll)]
    stat = jnp.zeros((heads, 128), F32)
    first = [items[0][0]] * unroll
    carry = (first, items[:unroll], later, items[-1], s_now, stat, stat)
    carry = lax.fori_loop(0, (total + unroll - 1) // unroll, body, carry)
    for n in range(unroll):
        flush(carry[0][n], n)


def suffix_part(q_rows, kv_suffix, seq_lens, heads, scale2, lat):
    rows, width = q_rows.shape
    seqs, _, slots = kv_suffix.shape
    size, depth, unroll = 512, 16, 4
    stat = jax.ShapeDtypeStruct((rows, 128), F32)
    return pl.pallas_call(
        functools.partial(suffix_kernel, scale2, lat, heads, unroll),
        out_shape=[jax.ShapeDtypeStruct((lat // 128, rows, 128), F32), stat, stat],
        in_specs=[SMEM, VMEM, HBM],
        out_specs=[VMEM, VMEM, VMEM],
        scratch_shapes=[pltpu.VMEM((-(-width // 128), rows, 128), F32), pltpu.VMEM((unroll, heads, lat), F32), pltpu.VMEM((depth, width, size), BF16), pltpu.SemaphoreType.DMA((depth,))],
        compiler_params=pltpu.CompilerParams(vmem_limit_bytes=32 * 2**20),
        cost_estimate=pl.CostEstimate(flops=2 * seqs * slots * 256 * 768, bytes_accessed=seqs * slots * width * 2, transcendentals=seqs * slots * heads),
        name='suffix',
    )(seq_lens, q_rows, kv_suffix)


def stats_of(ref, size):
    both = ref[size:size + 8, 0:size].T
    return both[:, 0:1], both[:, 1:2]


def output_kernel(hid_ref, os_ref, ms_ref, ls_ref, *refs):
    parts, (uv_ref, wo_ref, out_ref, v_buf) = refs[:3], refs[3:]
    rows, heads = hid_ref.shape[0], uv_ref.shape[0]
    lat, width = uv_ref.shape[1], uv_ref.shape[2]
    flat = rows * heads
    stats = [stats_of(ref, flat) for ref in parts]
    for h in range(heads):
        cut = slice(h * rows, (h + 1) * rows)
        m_s, l_s = ms_ref[cut, 0:1], jnp.sum(ls_ref[cut, :], axis=1, keepdims=True)
        ms = [m_s] + [m[cut] for m, _ in stats]
        ls = [l_s] + [l[cut] for _, l in stats]
        m_all = functools.reduce(jnp.maximum, ms)
        ws = [jnp.exp2(m - m_all) for m in ms]
        l_all = functools.reduce(jnp.add, [l * w for l, w in zip(ls, ws)])
        o_s = jnp.concatenate([os_ref[n, cut, :] for n in range(lat // 128)], axis=1)
        o_all = o_s * ws[0]
        for ref, w in zip(parts, ws[1:]):
            o_all = o_all + ref[cut, :] * w
        o_h = (o_all / l_all).astype(BF16)
        v_buf[:, h * width:(h + 1) * width] = jnp.dot(o_h, uv_ref[h], preferred_element_type=F32).astype(BF16)
    proj = jnp.dot(v_buf[...], wo_ref[...], preferred_element_type=F32)
    out_ref[...] = (hid_ref[...].astype(F32) + proj).astype(BF16)


def output_part(hidden, suffix, parts, w_uv, w_o):
    rows = hidden.shape[0]
    heads, lat, val = w_uv.shape
    return pl.pallas_call(
        output_kernel,
        out_shape=jax.ShapeDtypeStruct(hidden.shape, BF16),
        in_specs=[VMEM] * 9,
        out_specs=VMEM,
        scratch_shapes=[pltpu.VMEM((rows, heads * val), BF16)],
        compiler_params=pltpu.CompilerParams(vmem_limit_bytes=24 * 2**20),
        cost_estimate=pl.CostEstimate(flops=2 * rows * heads * val * (lat + hidden.shape[1]), bytes_accessed=2 * (w_uv.size + w_o.size), transcendentals=0),
        name='output',
    )(hidden, *suffix, *parts, w_uv, w_o)


def solution(mesh):
    group = mesh.shape['ctx']
    chips = group // CORES
    rows_spec = P(('dp', 'ctx'), None)
    whole_spec = P()

    def local_step(hidden, w_q, w_uk, w_uv, w_o, kv_prefix, kv_suffix, seq_lens):
        rows = hidden.shape[0]
        heads, nope, lat = w_uk.shape
        head_w = w_q.shape[1] // heads
        scale2 = head_w ** -0.5 * LOG2E
        kv_prefix = kv_prefix.T
        kv_suffix = kv_suffix.transpose(0, 2, 1)
        query, own, up, down = prefix_parts(hidden, seq_lens, w_q, w_uk, kv_prefix, scale2, chips)

        def send(value, hop):
            return lax.ppermute(value, 'ctx', [(j, (j + hop * CORES) % group) for j in range(group)])

        in_up, in_down = send(up, 1), send(down, -1)
        suffix = suffix_part(query, kv_suffix, seq_lens, heads, scale2, lat)
        return output_part(hidden, suffix, (own, in_up, in_down), w_uv, w_o)

    return jax.shard_map(local_step, mesh=mesh, in_specs=(rows_spec, whole_spec, whole_spec, whole_spec, whole_spec, rows_spec, P(('dp', 'ctx'), None, None), P(('dp', 'ctx'))), out_specs=rows_spec, check_vma=False)
```
